32 devices in a mesh: grid: 8 (over z, y), atom: 4 (over x, core).
Axes of the slice: x: 2, y: 2, z: 4, core: 2. Of those that a mesh axis runs over, the one named last changes fastest.
Arguments:
- weights: float32 [524288], P(('grid', 'atom')), may hold values from 0.25 to 4
- target: float32 [524288], P(('grid', 'atom')), may hold values from -6 to 6
- coupling: float32 [524288], P(('grid', 'atom')), may hold values from -0.9 to 0.9
- multipole_basis: float32 [25, 524288], P(None, ('grid', 'atom')), may hold values from -6 to 6
- rho_hist: float32 [8, 524288], P(None, ('grid', 'atom')), may hold values from -6 to 6
- res_hist: float32 [8, 524288], P(None, ('grid', 'atom')), may hold values from -6 to 6
- batch_atom: int32 [2048], P(('grid', 'atom')), may hold values from 0 to 2047
- owner_slot: int32 [2048], replicated, may hold values from 0 to 2047, each once
- slot_index: int32 [2], replicated, may hold values from 0 to 7
Outputs:
- density: float32 [524288], P(('grid', 'atom'))
- moments: float32 [25, 2048], P(None, 'atom')
The draws below stay inside these ranges and needn't reach their ends.
Inputs may be any that keep to these rules, and one draw needn't show every extreme that they name: `owner_slot`: each slot 0 to 2047 belongs to exactly one atom.
All inputs are finite; a program needn't handle non-finite values.
Results may differ from the reference program's by a relative error of at most 0.00011.
Values sent between devices are 32-bit elements; how exact they have to be, the bound alone decides.
A program may use at most 64 MiB of HBM per device.

```python
import math
import jax
import jax.numpy as jnp
import numpy as np
from jax import lax

H = 8
LM = 25
BATCH = 256
ITERS = 2
POINTS = 524288
BATCHES = 2048
ATOMS = 2048
ATOM_PTS = 256


def place_ends(result, key, least, largest):
    spot = [jax.random.randint(jax.random.fold_in(key, axis), (), 0, length) for axis, length in enumerate(result.shape)]
    longest = result.shape.index(max(result.shape))
    neighbour = spot[:longest] + [(spot[longest] + 1) % result.shape[longest]] + spot[longest + 1:]
    return result.at[tuple(spot)].set(least).at[tuple(neighbour)].set(largest)


def levels(own_key, dims, pieces, smallest, top_value):
    def one(position, shards_of):
        heights = jax.random.uniform(jax.random.fold_in(jax.random.fold_in(own_key, 6), position), (shards_of,), jnp.float32, smallest / len(pieces), top_value / len(pieces))
        return jnp.repeat(jnp.exp(heights), dims[position] // shards_of).reshape((-1,) + (1,) * (len(dims) - position - 1))

    gain = one(*pieces[0])
    for cut in pieces[1:]:
        gain = gain * one(*cut)
    return gain


def noise(stream_key, shape, scale, reach, shards=(), held_as=jnp.bfloat16):
    gain = levels(stream_key, shape, shards, -0.22, 0.18) if shards else 1.0
    entries = jax.random.normal(stream_key, shape, jnp.float32) * scale * gain
    return jnp.minimum(jnp.maximum(entries, -reach), reach).astype(held_as)


def setup_inputs(seed: int = 0) -> dict:
    splits = jax.random.split(jax.random.key(seed), 10)
    return {
        "weights": jnp.clip(jnp.exp(math.log(4.0) - 2.7725887 * jax.random.uniform(splits[0], (POINTS,), jnp.float32) ** levels(splits[0], (POINTS,), ((0, 32),), -0.2, 0.2)), 0.25, 4.0),
        "target": noise(splits[1], (POINTS,), 1.0, 6.0, ((0, 32),), jnp.float32),
        "coupling": jnp.clip(jax.random.uniform(splits[2], (POINTS,), jnp.float32, -0.9, 0.9) * levels(splits[2], (POINTS,), ((0, 32),), -0.4, 0.0), -0.9, 0.9),
        "multipole_basis": noise(splits[3], (LM, POINTS), 1.0, 6.0, ((1, 32),), jnp.float32),
        "rho_hist": noise(splits[4], (H, POINTS), 1.0, 6.0, ((1, 32),), jnp.float32),
        "res_hist": noise(splits[5], (H, POINTS), 1.0, 6.0, ((1, 32),), jnp.float32),
        "batch_atom": place_ends(jax.random.randint(splits[6], (BATCHES,), 0, ATOMS), jax.random.fold_in(splits[6], 1), 0, ATOMS - 1).astype(jnp.int32),
        "owner_slot": jax.random.permutation(splits[7], ATOMS).astype(jnp.int32),
        "slot_index": jax.random.randint(splits[8], (ITERS,), 0, H).astype(jnp.int32),
    }


damping_table = np.array([1.0 / (1 + degree) for degree in range(5) for order in range(2 * degree + 1)], dtype=np.float32)
mixing_beta = 0.5
ridge_share = 0.1

def mixing_weights(intersect):
    hist_len = intersect.shape[0]
    ridge_val = ridge_share * jnp.trace(intersect) / hist_len
    shifted = intersect + ridge_val * jnp.eye(hist_len, dtype=intersect.dtype)
    factor = jnp.linalg.cholesky(shifted)
    forward = []
    for row_at in range(hist_len):
        entry_val = 1.0
        for col_at in range(row_at):
            entry_val = entry_val - factor[row_at, col_at] * forward[col_at]
        forward.append(entry_val / factor[row_at, row_at])
    backward = [None] * hist_len
    for row_at in reversed(range(hist_len)):
        entry_val = forward[row_at]
        for col_at in range(row_at + 1, hist_len):
            entry_val = entry_val - factor[col_at, row_at] * backward[col_at]
        backward[row_at] = entry_val / factor[row_at, row_at]
    solved = jnp.stack(backward)
    return solved / jnp.sum(solved)

def reference(weights, target, coupling, multipole_basis, rho_hist, res_hist, batch_atom, owner_slot, slot_index):
    hi_prec = lax.Precision.HIGHEST
    damping = jnp.asarray(damping_table, dtype=weights.dtype)
    batch_slot = owner_slot[batch_atom].astype(jnp.int32)
    basis_blocks = multipole_basis.reshape(LM, BATCHES, BATCH)
    density = None
    moments = None
    for iteration in range(ITERS):
        intersect = jnp.dot(res_hist * weights[None, :], res_hist.T, precision=hi_prec)
        coeffs = mixing_weights(intersect)
        rho_mix = jnp.dot(coeffs, rho_hist, precision=hi_prec)
        res_mix = jnp.dot(coeffs, res_hist, precision=hi_prec)
        per_batch = lax.optimization_barrier(jnp.sum((weights * res_mix).reshape(1, BATCHES, BATCH) * basis_blocks, axis=2))
        moments = jax.ops.segment_sum(per_batch.T, batch_slot, num_segments=ATOMS).T / jnp.sqrt(jnp.float32(ATOM_PTS)).astype(weights.dtype)
        at_batch = damping[:, None] * moments[:, batch_slot]
        correct = lax.optimization_barrier(jnp.sum(at_batch[:, :, None] * basis_blocks, axis=0)).reshape(POINTS)
        density = rho_mix + mixing_beta * (res_mix - correct)
        res_new = target + coupling * jnp.tanh(density) - density
        where = slot_index[iteration]
        rho_hist = rho_hist.at[where].set(density)
        res_hist = res_hist.at[where].set(res_new)
    return (density, moments)
```

```python
import functools
import math

import jax
import jax.numpy as jnp
from jax import lax
from jax.experimental import pallas as pl
from jax.experimental.pallas import tpu as pltpu
from jax.sharding import PartitionSpec as P

MESH = pl.DeviceIdType.MESH
LANES = 128
SUBS = 8
mixing_beta = 0.5
ridge_share = 0.1
F32 = jnp.float32


def solve_coeffs(entry, hist_len):
    trace = entry[0][0]
    for i in range(1, hist_len):
        trace = trace + entry[i][i]
    ridge = (ridge_share / hist_len) * trace
    low = [[entry[i][j] for j in range(i + 1)] for i in range(hist_len)]
    for i in range(hist_len):
        low[i][i] = low[i][i] + ridge
    inverse = [None] * hist_len
    factor = [[None] * hist_len for _ in range(hist_len)]
    forward = [jnp.ones_like(trace) for _ in range(hist_len)]
    for j in range(hist_len):
        inverse[j] = 1.0 / low[j][j]
        for i in range(j + 1, hist_len):
            factor[i][j] = low[i][j] * inverse[j]
        for i in range(j + 1, hist_len):
            forward[i] = forward[i] - factor[i][j] * forward[j]
            for k in range(j + 1, i + 1):
                low[i][k] = low[i][k] - factor[i][j] * low[k][j]
    backward = [forward[i] * inverse[i] for i in range(hist_len)]
    for j in reversed(range(hist_len)):
        for i in range(j):
            backward[i] = backward[i] - factor[j][i] * backward[j]
    total = backward[0]
    for i in range(1, hist_len):
        total = total + backward[i]
    return [backward[i] / total for i in range(hist_len)]


def split(x):
    pieces = []
    for _ in range(2):
        piece = x.astype(jnp.bfloat16).astype(F32)
        pieces.append(piece)
        x = x - piece
    return pieces


def kernel(
    cfg,
    batch_atom_hbm,
    owner_slot_hbm,
    slot_index_hbm,
    w_hbm,
    target_hbm,
    coupling_hbm,
    basis_hbm,
    rho_hbm,
    res_hbm,
    density_out,
    moments_out,
    w,
    target,
    coupling,
    basis,
    rho,
    res,
    fresh,
    fresh_w,
    row_bufs,
    moment_bufs,
    near,
    own,
    hist_moments,
    base_rows,
    correct,
    batch_atom,
    owner_slot,
    slot_index,
    load_sem,
    send_sem,
    recv_sem,
):
    iters, hist_len, harmonics, batches, width, owned, groups, members, scale = cfg
    devices = groups * members
    tiles = w.shape[0]
    per_batch = width // LANES
    half = LANES // 2
    rows = batches // 4
    my_group = lax.axis_index("grid")
    my_member = lax.axis_index("atom")
    me = my_group * members + my_member

    def peer(step):
        spot = lax.rem(me + step, devices)
        return (lax.div(spot, members), lax.rem(spot, members))

    barrier = pltpu.get_barrier_semaphore()

    loads = [
        pltpu.make_async_copy(src, dst, load_sem.at[k])
        for k, (src, dst) in enumerate(
            (
                (res_hbm, res),
                (w_hbm, w),
                (basis_hbm, basis),
                (rho_hbm, rho),
                (target_hbm, target),
                (coupling_hbm, coupling),
                (batch_atom_hbm, batch_atom),
                (owner_slot_hbm, owner_slot),
                (slot_index_hbm, slot_index),
            )
        )
    ]
    for k in (6, 7, 0, 1):
        loads[k].start()

    @pl.loop(1, devices)
    def _(step):
        pl.semaphore_signal(barrier, inc=1, device_id=peer(step), device_id_type=MESH)

    for k in (2, 3, 4, 5, 8):
        loads[k].start()
    loads[6].wait()
    loads[7].wait()

    lane = lax.broadcasted_iota(jnp.int32, (SUBS, LANES), 1)
    sub = lax.broadcasted_iota(jnp.int32, (SUBS, LANES), 0)
    quarter = lane // 32
    lane_row = lax.broadcasted_iota(jnp.int32, (1, LANES), 1)

    slot_row = jnp.zeros((1, LANES), F32)
    slot_cols = []
    for block in range(batches // SUBS):
        col = jnp.zeros((SUBS, LANES), F32)
        for at in range(SUBS):
            b = block * SUBS + at
            slot = owner_slot[batch_atom[b]].astype(F32)
            slot_row = jnp.where(lane_row == half + b, slot, slot_row)
            col = jnp.where(sub == at, slot, col)
        slot_cols.append(col)
    slot_col = jnp.concatenate(slot_cols, axis=0)

    def lane_tile(t):
        return pl.ds(pl.multiple_of(t * LANES, LANES), LANES)

    def exchange(buf, which):
        def copy(ref, step):
            return pltpu.make_async_remote_copy(
                src_ref=ref,
                dst_ref=ref,
                send_sem=send_sem.at[which],
                recv_sem=recv_sem.at[which],
                device_id=peer(step),
                device_id_type=MESH,
            )

        @pl.loop(1, devices)
        def _(step):
            copy(buf.at[me], step).start()

        def wait():
            everyone = copy(buf.at[pl.ds(0, devices - 1)], 1)
            everyone.wait_recv()
            everyone.wait_send()

        return wait

    def total_row(buf):
        total = buf[0]
        for spot in range(1, devices):
            total = total + buf[spot]
        return total

    def splat(row, k):
        return jnp.broadcast_to(row[:, k : k + 1], (1, LANES))

    shifts = hist_len // 2 + 1
    entry = None
    for iteration in range(iters):
        row_buf = row_bufs.at[iteration]
        moment_buf = moment_bufs.at[iteration]
        last = iteration == iters - 1

        if iteration == 0:
            loads[0].wait()
            loads[1].wait()

            def gram(step, acc):
                acc = list(acc)
                for u in range(8):
                    t = step * 8 + u
                    x = res[:, lane_tile(t)]
                    y = x * w[pl.ds(t, 1), :]
                    for r in range(shifts):
                        acc[r] = acc[r] + y * (pltpu.roll(x, r, 0) if r else x)
                return tuple(acc)

            acc = lax.fori_loop(0, tiles // 8, gram, tuple(jnp.zeros((SUBS, LANES), F32) for _ in range(shifts)))
            packed = jnp.zeros((SUBS, LANES), F32)
            for r in range(shifts):
                packed = jnp.where(lane == hist_len * r + sub, jnp.sum(acc[r], axis=1, keepdims=True), packed)
            row_buf[pl.ds(me, 1)] = (jnp.sum(packed, axis=0, keepdims=True) + slot_row)[None]
            pl.semaphore_wait(barrier, devices - 1)
        else:
            slot = slot_index[iteration - 1]
            replaced = sub == slot

            def refresh(step, acc):
                for u in range(8):
                    t = step * 8 + u
                    new_res = jnp.where(replaced, fresh[pl.ds(t, 1), :], res[:, lane_tile(t)])
                    new_rho = jnp.where(replaced, density_out[pl.ds(t, 1), :], rho[:, lane_tile(t)])
                    res[:, lane_tile(t)] = new_res
                    rho[:, lane_tile(t)] = new_rho
                    acc = acc + fresh_w[pl.ds(t, 1), :] * new_res
                return acc

            acc = lax.fori_loop(0, tiles // 8, refresh, jnp.zeros((SUBS, LANES), F32))
            packed = jnp.where(lane == sub, jnp.sum(acc, axis=1, keepdims=True), 0.0)
            row_buf[pl.ds(me, 1)] = jnp.sum(packed, axis=0, keepdims=True)[None]
        wait = exchange(row_buf, 2 * iteration)

        if iteration == 0:
            loads[2].wait()

        @pl.loop(0, rows)
        def _(r):
            xs, ys = [], []
            for q in range(4):
                b = q * rows + r
                at = pl.ds(pl.multiple_of(b * width, width), width)
                gain = jnp.concatenate([w[pl.ds(b * per_batch + v, 1), :] for v in range(per_batch)], axis=1)
                xs.extend(split(res[:, at] * gain))
                ys.append(jnp.concatenate([basis[0:24, at], jnp.broadcast_to(basis[24:25, at], (SUBS, width))], axis=0))
            x = jnp.concatenate(xs, axis=0).astype(jnp.bfloat16)
            out = None
            for y in split(jnp.concatenate(ys, axis=0)):
                part = lax.dot_general(
                    x, y.astype(jnp.bfloat16), (((1,), (1,)), ((), ())), preferred_element_type=F32
                )
                out = part if out is None else out + part
            tile = jnp.zeros((SUBS, LANES), F32)
            for q in range(4):
                block = out[16 * q : 16 * q + 8] + out[16 * q + 8 : 16 * q + 16]
                tile = jnp.where(quarter == q, block, tile)
            hist_moments[r] = tile

        wait()

        row = total_row(row_buf)
        if iteration == 0:
            entry = [[None] * (i + 1) for i in range(hist_len)]
            for i in range(hist_len):
                for j in range(i + 1):
                    r = i - j
                    at = hist_len * r + i if r < shifts else hist_len * (hist_len - r) + j
                    entry[i][j] = splat(row, at)
        else:
            news = [splat(row, k) for k in range(hist_len)]
            slot_vec = jnp.zeros((1, LANES), jnp.int32) + slot
            entry = [
                [
                    jnp.where(slot_vec == i, news[j], jnp.where(slot_vec == j, news[i], entry[i][j]))
                    for j in range(i + 1)
                ]
                for i in range(hist_len)
            ]
        coeffs = solve_coeffs(entry, hist_len)
        coeff_col = jnp.zeros((SUBS, LANES), F32)
        for i in range(hist_len):
            coeff_col = jnp.where(sub == i, coeffs[i], coeff_col)

        mixed = [jnp.sum(coeff_col * hist_moments[r], axis=0, keepdims=True) for r in range(rows)]
        moment_buf[pl.ds(me, 1)] = jnp.concatenate(mixed, axis=0)[None]
        wait = exchange(moment_buf, 2 * iteration + 1)

        if iteration == 0:
            base = (my_member * owned).astype(F32)
            wide = lax.broadcasted_iota(jnp.int32, (owned, LANES), 0).astype(F32) + base

            @pl.loop(0, devices // SUBS)
            def _(c):
                ids = jnp.concatenate([row_buf[c * SUBS + i] for i in range(SUBS)], axis=0)
                stepped = pltpu.roll(ids, 0, 1, stride=rows, stride_axis=0)
                for q in range(4):
                    turned = pltpu.roll(stepped, (half - rows * q) % LANES, 1)
                    slots = jnp.sum(jnp.where(lane // rows == sub, turned, 0.0), axis=0, keepdims=True)
                    near[q * batches : (q + 1) * batches, lane_tile(c)] = jnp.where(
                        slot_col == slots, 1.0, 0.0
                    ).astype(jnp.bfloat16)
                    own[q * owned : (q + 1) * owned, lane_tile(c)] = jnp.where(wide == slots, 1.0, 0.0).astype(
                        jnp.bfloat16
                    )

            for k in (3, 4, 5, 8):
                loads[k].wait()

        def base_step(step, carry):
            for u in range(8):
                t = step * 8 + u
                part = coeff_col * (rho[:, lane_tile(t)] + mixing_beta * res[:, lane_tile(t)])
                base_rows[pl.ds(t, 1), :] = jnp.sum(part, axis=0, keepdims=True)
            return carry

        lax.fori_loop(0, tiles // 8, base_step, 0)
        wait()

        everywhere = moment_buf[...].reshape(devices * rows, LANES)
        pieces = jnp.concatenate([piece.astype(jnp.bfloat16) for piece in split(everywhere)], axis=1)

        def gathered(mask, count):
            out = jnp.dot(mask[...], pieces, preferred_element_type=F32)
            out = out[:, 0:LANES] + out[:, LANES:]
            group = lax.broadcasted_iota(jnp.int32, (count, LANES), 1) // 32
            total = out[0:count]
            for q in range(1, 4):
                total = jnp.where(group == q, out[q * count : (q + 1) * count], total)
            total = total + pltpu.roll(total, 64, 1)
            total = total + pltpu.roll(total, 32, 1)
            return jnp.transpose(jnp.concatenate([total] * max(1, LANES // count), axis=0))[0:32] * scale

        at_batch = gathered(near, batches)
        comp = lax.broadcasted_iota(jnp.int32, (32, LANES), 0)
        degree = sum((comp >= (l + 1) * (l + 1)).astype(F32) for l in range(4))
        damped = jnp.where(comp < harmonics, at_batch * (mixing_beta / (1.0 + degree)), 0.0)

        def density_step(step, ahead):
            for u in range(16):
                b = step * 16 + u
                col = jnp.broadcast_to(ahead[:, u : u + 1], (32, LANES))
                for v in range(per_batch):
                    t = b * per_batch + v
                    part = col[24:32] * basis[24:25, lane_tile(t)]
                    for g in range(3):
                        part = part + col[g * SUBS : (g + 1) * SUBS] * basis[g * SUBS : (g + 1) * SUBS, lane_tile(t)]
                    correct[pl.ds(t, 1), :] = jnp.sum(part, axis=0, keepdims=True)
            return pltpu.roll(ahead, LANES - 16, 1)

        lax.fori_loop(0, batches // 16, density_step, damped)
        density = base_rows[...] - correct[...]
        density_out[...] = density
        if last:
            moments_out[...] = gathered(own, owned)[0:harmonics]
        else:
            new = target[...] + coupling[...] * jnp.tanh(density) - density
            fresh[...] = new
            fresh_w[...] = new * w[...]


def finish(density, moments, density_out, moments_out, sem):
    copies = [
        pltpu.make_async_copy(density, density_out, sem.at[0]),
        pltpu.make_async_copy(moments, moments_out, sem.at[1]),
    ]
    for copy in copies:
        copy.start()
    for copy in copies:
        copy.wait()


def local(weights, target, coupling, multipole_basis, rho_hist, res_hist, batch_atom, owner_slot, slot_index):
    harmonics, points = multipole_basis.shape
    hist_len = res_hist.shape[0]
    batches = batch_atom.shape[0]
    groups = lax.axis_size("grid")
    members = lax.axis_size("atom")
    devices = groups * members
    owned = owner_slot.shape[0] // members
    scale = 1.0 / math.sqrt(points * groups // owned)
    iters = slot_index.shape[0]
    cfg = (iters, hist_len, harmonics, batches, points // batches, owned, groups, members, scale)
    tiles = points // LANES
    flat = (tiles, LANES)
    any_space = pl.BlockSpec(memory_space=pl.ANY)
    vmem = pl.BlockSpec(memory_space=pltpu.VMEM)
    density, moments = pl.pallas_call(
        functools.partial(kernel, cfg),
        out_shape=(jax.ShapeDtypeStruct(flat, F32), jax.ShapeDtypeStruct((harmonics, owned), F32)),
        in_specs=[any_space] * 9,
        out_specs=(vmem, vmem),
        scratch_shapes=[
            pltpu.VMEM(flat, F32),
            pltpu.VMEM(flat, F32),
            pltpu.VMEM(flat, F32),
            pltpu.VMEM((harmonics, points), F32),
            pltpu.VMEM((hist_len, points), F32),
            pltpu.VMEM((hist_len, points), F32),
            pltpu.VMEM(flat, F32),
            pltpu.VMEM(flat, F32),
            pltpu.VMEM((iters, devices, 1, LANES), F32),
            pltpu.VMEM((iters, devices, batches // 4, LANES), F32),
            pltpu.VMEM((4 * batches, devices * batches // 4), jnp.bfloat16),
            pltpu.VMEM((4 * owned, devices * batches // 4), jnp.bfloat16),
            pltpu.VMEM((batches // 4, SUBS, LANES), F32),
            pltpu.VMEM(flat, F32),
            pltpu.VMEM(flat, F32),
            pltpu.SMEM(batch_atom.shape, batch_atom.dtype),
            pltpu.SMEM(owner_slot.shape, owner_slot.dtype),
            pltpu.SMEM(slot_index.shape, slot_index.dtype),
            pltpu.SemaphoreType.DMA((9,)),
            pltpu.SemaphoreType.DMA((2 * iters,)),
            pltpu.SemaphoreType.DMA((2 * iters,)),
        ],
        compiler_params=pltpu.CompilerParams(
            collective_id=0, has_side_effects=True, vmem_limit_bytes=40 * 1024 * 1024
        ),
    )(
        *(
            pltpu.with_memory_space_constraint(x, pltpu.HBM)
            for x in (
                batch_atom,
                owner_slot,
                slot_index,
                weights.reshape(flat),
                target.reshape(flat),
                coupling.reshape(flat),
                multipole_basis,
                rho_hist,
                res_hist,
            )
        )
    )
    density, moments = pl.pallas_call(
        finish,
        out_shape=(jax.ShapeDtypeStruct(flat, F32), jax.ShapeDtypeStruct((harmonics, owned), F32)),
        in_specs=[vmem] * 2,
        out_specs=(any_space, any_space),
        scratch_shapes=[pltpu.SemaphoreType.DMA((2,))],
    )(*(pltpu.with_memory_space_constraint(x, pltpu.VMEM) for x in (density, moments)))
    return density.reshape(points), moments


def solution(mesh):
    both = ("grid", "atom")
    placed = (P(both), P(both), P(both), P(None, both), P(None, both), P(None, both), P(both), P(), P())
    return jax.shard_map(
        local,
        mesh=mesh,
        in_specs=placed,
        out_specs=(P(both), P(None, "atom")),
        check_vma=False,
    )
```

```python
import functools
import math

import jax
import jax.numpy as jnp
from jax import lax
from jax.experimental import pallas as pl
from jax.experimental.pallas import tpu as pltpu
from jax.sharding import PartitionSpec as P

MESH = pl.DeviceIdType.MESH
LANES = 128
SUBS = 8
mixing_beta = 0.5
ridge_share = 0.1
F32 = jnp.float32


def solve_coeffs(entry, hist_len):
    trace = entry[0][0]
    for i in range(1, hist_len):
        trace = trace + entry[i][i]
    ridge = (ridge_share / hist_len) * trace
    low = [[entry[i][j] for j in range(i + 1)] for i in range(hist_len)]
    for i in range(hist_len):
        low[i][i] = low[i][i] + ridge
    inverse = [None] * hist_len
    factor = [[None] * hist_len for _ in range(hist_len)]
    forward = [jnp.ones_like(trace) for _ in range(hist_len)]
    for j in range(hist_len):
        inverse[j] = 1.0 / low[j][j]
        for i in range(j + 1, hist_len):
            factor[i][j] = low[i][j] * inverse[j]
        for i in range(j + 1, hist_len):
            forward[i] = forward[i] - factor[i][j] * forward[j]
            for k in range(j + 1, i + 1):
                low[i][k] = low[i][k] - factor[i][j] * low[k][j]
    backward = [forward[i] * inverse[i] for i in range(hist_len)]
    for j in reversed(range(hist_len)):
        for i in range(j):
            backward[i] = backward[i] - factor[j][i] * backward[j]
    total = backward[0]
    for i in range(1, hist_len):
        total = total + backward[i]
    return [backward[i] / total for i in range(hist_len)]


def split(x):
    pieces = []
    for _ in range(2):
        piece = x.astype(jnp.bfloat16).astype(F32)
        pieces.append(piece)
        x = x - piece
    return pieces


def flips(value, count):
    out = []
    bit = 1
    while bit < count:
        out.append(bit - 2 * bit * lax.rem(lax.div(value, bit), 2))
        bit *= 2
    return out


def flipped(value, changes, mask):
    for k, change in enumerate(changes):
        if mask >> k & 1:
            value = value + change
    return value


def stacked_sums(parts, sub):
    low = sub % 8 < 4
    halves = [
        jnp.where(low, parts[t], parts[t + 4]) + pltpu.roll(jnp.where(low, parts[t + 4], parts[t]), 4, 0)
        for t in range(4)
    ]
    low = sub % 4 < 2
    quarters = [
        jnp.where(low, halves[t] + pltpu.roll(halves[t], 6, 0), halves[t + 2] + pltpu.roll(halves[t + 2], 2, 0))
        for t in range(2)
    ]
    low = sub % 2 < 1
    return jnp.where(
        low, quarters[0] + pltpu.roll(quarters[0], 7, 0), quarters[1] + pltpu.roll(quarters[1], 1, 0)
    )


def kernel(
    cfg,
    batch_atom_hbm,
    owner_slot_hbm,
    slot_index_hbm,
    w_hbm,
    target_hbm,
    coupling_hbm,
    basis_hbm,
    rho_hbm,
    res_hbm,
    density_out,
    moments_out,
    w,
    target,
    coupling,
    basis,
    rho,
    res,
    fresh,
    fresh_w,
    row_bufs,
    sent_moments,
    all_moments,
    near,
    own,
    own_sum,
    hist_moments,
    base_rows,
    correct,
    batch_atom,
    owner_slot,
    slot_index,
    load_sem,
    row_sem,
    moment_sem,
):
    iters, hist_len, harmonics, batches, width, owned, groups, members, scale = cfg
    devices = groups * members
    tiles = w.shape[0]
    per_batch = width // LANES
    half = LANES // 2
    rows = batches // 4
    my_group = lax.axis_index("grid")
    my_member = lax.axis_index("atom")
    me = my_group * members + my_member
    chips = devices // 2
    upper = chips // 2
    chip = lax.div(me, 2)
    core = lax.rem(me, 2)
    group_flips = flips(my_group, groups)
    member_flips = flips(my_member, members)

    def peer(step):
        return (
            flipped(my_group, group_flips, step // members),
            flipped(my_member, member_flips, step % members),
        )

    plane = min(chips, (members // 2) ** 2)
    chip_steps = [z * plane + p for p in reversed(range(plane)) for z in reversed(range(chips // plane))]
    device_steps = [2 * step + c for step in chip_steps for c in (1, 0)][:-1]

    barrier = pltpu.get_barrier_semaphore()

    loads = [
        pltpu.make_async_copy(src, dst, load_sem.at[k])
        for k, (src, dst) in enumerate(
            (
                (res_hbm, res),
                (w_hbm, w),
                (basis_hbm, basis),
                (rho_hbm, rho),
                (target_hbm, target),
                (coupling_hbm, coupling),
                (batch_atom_hbm, batch_atom),
                (owner_slot_hbm, owner_slot),
                (slot_index_hbm, slot_index),
            )
        )
    ]
    for k in (6, 7, 0, 1):
        loads[k].start()

    for step in device_steps:
        pl.semaphore_signal(barrier, inc=1, device_id=peer(step), device_id_type=MESH)

    for k in (2, 3, 4, 5, 8):
        loads[k].start()
    loads[6].wait()
    loads[7].wait()

    lane = lax.broadcasted_iota(jnp.int32, (SUBS, LANES), 1)
    sub = lax.broadcasted_iota(jnp.int32, (SUBS, LANES), 0)
    quarter = lane // 32
    lane_row = lax.broadcasted_iota(jnp.int32, (1, LANES), 1)

    slot_row = jnp.zeros((1, LANES), F32)
    slot_cols = []
    for block in range(batches // SUBS):
        col = jnp.zeros((SUBS, LANES), F32)
        for at in range(SUBS):
            b = block * SUBS + at
            slot = owner_slot[batch_atom[b]].astype(F32)
            slot_row = jnp.where(lane_row == half + b, slot, slot_row)
            col = jnp.where(sub == at, slot, col)
        slot_cols.append(col)
    slot_col = jnp.concatenate(slot_cols, axis=0)

    def lane_tile(t):
        return pl.ds(pl.multiple_of(t * LANES, LANES), LANES)

    def remote(src, dst, sems, step):
        return pltpu.make_async_remote_copy(
            src_ref=src,
            dst_ref=dst,
            send_sem=sems.at[0],
            recv_sem=sems.at[1],
            device_id=peer(step),
            device_id_type=MESH,
        )

    def exchange_rows(buf, sems):
        for step in device_steps:
            remote(buf.at[me], buf.at[me], sems, step).start()

        def wait():
            others = buf.at[pl.ds(0, devices - 1)]
            everyone = remote(others, others, sems, 1)
            everyone.wait_recv()
            everyone.wait_send()

        return wait

    def exchange_moments(mine, buf, sems):
        halves = [pl.ds((upper * k + chip - lax.rem(chip, upper)) % chips, upper) for k in range(2)]
        remote(mine, buf.at[0, chip], sems.at[0], 1).start()
        for step in chip_steps[:-1]:
            remote(mine, buf.at[0, chip], sems.at[step // upper], 2 * step + 1).start()
        landed = [remote(buf.at[0, half], buf.at[0, half], sems.at[k], 1) for k, half in enumerate(halves)]
        passed = [remote(buf.at[0, half], buf.at[1, half], sems.at[2 + k], 1) for k, half in enumerate(halves)]

        def wait_landed():
            for k in range(2):
                landed[k].wait_recv()
                passed[k].start()

        def wait_passed():
            for k in range(2):
                passed[k].wait_recv()
            for k in range(2):
                landed[k].wait_send()
                passed[k].wait_send()

        return wait_landed, wait_passed

    def total_row(buf):
        total = buf[0]
        for spot in range(1, devices):
            total = total + buf[spot]
        return total

    def splat(row, k):
        return jnp.broadcast_to(row[:, k : k + 1], (1, LANES))

    shifts = hist_len // 2 + 1
    entry = None
    for iteration in range(iters):
        row_buf = row_bufs.at[iteration]
        sent_buf = sent_moments.at[iteration]
        moment_buf = all_moments.at[iteration]
        last = iteration == iters - 1

        if iteration == 0:
            loads[0].wait()
            loads[1].wait()

            def gram(step, acc):
                acc = list(acc)
                for u in range(8):
                    t = step * 8 + u
                    x = res[:, lane_tile(t)]
                    y = x * w[pl.ds(t, 1), :]
                    for r in range(shifts):
                        acc[r] = acc[r] + y * (pltpu.roll(x, r, 0) if r else x)
                return tuple(acc)

            acc = lax.fori_loop(0, tiles // 8, gram, tuple(jnp.zeros((SUBS, LANES), F32) for _ in range(shifts)))
            packed = jnp.zeros((SUBS, LANES), F32)
            for r in range(shifts):
                packed = jnp.where(lane == hist_len * r + sub, jnp.sum(acc[r], axis=1, keepdims=True), packed)
            row_buf[pl.ds(me, 1)] = (jnp.sum(packed, axis=0, keepdims=True) + slot_row)[None]
            pl.semaphore_wait(barrier, devices - 1)
        else:
            slot = slot_index[iteration - 1]
            replaced = sub == slot

            def inner(step, acc):
                acc = list(acc)
                for u in range(16):
                    t = step * 16 + u
                    acc[u % 4] = acc[u % 4] + fresh_w[pl.ds(t, 1), :] * res[:, lane_tile(t)]
                return tuple(acc)

            acc = lax.fori_loop(0, tiles // 16, inner, tuple(jnp.zeros((SUBS, LANES), F32) for _ in range(4)))
            acc = (acc[0] + acc[1]) + (acc[2] + acc[3])
            acc = jnp.where(replaced, square, acc)
            packed = jnp.where(lane == sub, jnp.sum(acc, axis=1, keepdims=True), 0.0)
            row_buf[pl.ds(me, 1)] = jnp.sum(packed, axis=0, keepdims=True)[None]
        wait = exchange_rows(row_buf, row_sem.at[iteration])

        if iteration == 0:
            loads[2].wait()
        else:

            @pl.loop(0, tiles // 8)
            def _(step):
                for u in range(8):
                    t = step * 8 + u
                    res[:, lane_tile(t)] = jnp.where(replaced, fresh[pl.ds(t, 1), :], res[:, lane_tile(t)])
                    rho[:, lane_tile(t)] = jnp.where(replaced, density_out[pl.ds(t, 1), :], rho[:, lane_tile(t)])

        @pl.loop(0, rows)
        def _(r):
            xs, ys = [], []
            for q in range(4):
                b = q * rows + r
                at = pl.ds(pl.multiple_of(b * width, width), width)
                gain = jnp.concatenate([w[pl.ds(b * per_batch + v, 1), :] for v in range(per_batch)], axis=1)
                xs.extend(split(res[:, at] * gain))
                ys.append(jnp.concatenate([basis[0:24, at], jnp.broadcast_to(basis[24:25, at], (SUBS, width))], axis=0))
            x = jnp.concatenate(xs, axis=0).astype(jnp.bfloat16)
            out = None
            for y in split(jnp.concatenate(ys, axis=0)):
                part = lax.dot_general(
                    x, y.astype(jnp.bfloat16), (((1,), (1,)), ((), ())), preferred_element_type=F32
                )
                out = part if out is None else out + part
            tile = jnp.zeros((SUBS, LANES), F32)
            for q in range(4):
                block = out[16 * q : 16 * q + 8] + out[16 * q + 8 : 16 * q + 16]
                tile = jnp.where(quarter == q, block, tile)
            hist_moments[r] = tile

        wait()

        row = total_row(row_buf)
        if iteration == 0:
            entry = [[None] * (i + 1) for i in range(hist_len)]
            for i in range(hist_len):
                for j in range(i + 1):
                    r = i - j
                    at = hist_len * r + i if r < shifts else hist_len * (hist_len - r) + j
                    entry[i][j] = splat(row, at)
        else:
            news = [splat(row, k) for k in range(hist_len)]
            slot_vec = jnp.zeros((1, LANES), jnp.int32) + slot
            entry = [
                [
                    jnp.where(slot_vec == i, news[j], jnp.where(slot_vec == j, news[i], entry[i][j]))
                    for j in range(i + 1)
                ]
                for i in range(hist_len)
            ]
        coeffs = solve_coeffs(entry, hist_len)
        coeff_col = jnp.zeros((SUBS, LANES), F32)
        for i in range(hist_len):
            coeff_col = jnp.where(sub == i, coeffs[i], coeff_col)

        mixed = [jnp.sum(coeff_col * hist_moments[r], axis=0, keepdims=True) for r in range(rows)]
        sent_buf[...] = jnp.concatenate(mixed, axis=0)
        wait_landed, wait_passed = exchange_moments(sent_buf, moment_buf, moment_sem.at[iteration])

        if iteration == 0:
            base = (my_member * owned).astype(F32)
            wide = lax.broadcasted_iota(jnp.int32, (owned, LANES), 0).astype(F32) + base

            @pl.loop(0, devices // SUBS)
            def _(c):
                side = lax.div(c, chips // SUBS)
                first = 2 * SUBS * lax.rem(c, chips // SUBS) + lax.rem(core + 1 + side, 2)
                ids = jnp.concatenate([row_buf[first + 2 * i] for i in range(SUBS)], axis=0)
                stepped = pltpu.roll(ids, 0, 1, stride=rows, stride_axis=0)
                for q in range(4):
                    turned = pltpu.roll(stepped, (half - rows * q) % LANES, 1)
                    slots = jnp.sum(jnp.where(lane // rows == sub, turned, 0.0), axis=0, keepdims=True)
                    near[q * batches : (q + 1) * batches, lane_tile(c)] = jnp.where(
                        slot_col == slots, 1.0, 0.0
                    ).astype(jnp.bfloat16)
                    own[q * owned : (q + 1) * owned, lane_tile(c)] = jnp.where(wide == slots, 1.0, 0.0).astype(
                        jnp.bfloat16
                    )

            for k in (3, 4, 5, 8):
                loads[k].wait()

        def base_step(step, carry):
            for u in range(8):
                t = step * 8 + u
                part = coeff_col * (rho[:, lane_tile(t)] + mixing_beta * res[:, lane_tile(t)])
                base_rows[pl.ds(t, 1), :] = jnp.sum(part, axis=0, keepdims=True)
            return carry

        lax.fori_loop(0, tiles // 8, base_step, 0)
        depth = chips * rows

        def gathered(mask, count, side):
            everywhere = moment_buf[side].reshape(depth, LANES)
            pieces = jnp.concatenate([piece.astype(jnp.bfloat16) for piece in split(everywhere)], axis=1)
            out = jnp.dot(mask[:, side * depth : (side + 1) * depth], pieces, preferred_element_type=F32)
            out = out[:, 0:LANES] + out[:, LANES:]
            group = lax.broadcasted_iota(jnp.int32, (count, LANES), 1) // 32
            total = out[0:count]
            for q in range(1, 4):
                total = jnp.where(group == q, out[q * count : (q + 1) * count], total)
            return total

        def folded(total, count):
            total = total + pltpu.roll(total, 64, 1)
            total = total + pltpu.roll(total, 32, 1)
            return jnp.transpose(jnp.concatenate([total] * max(1, LANES // count), axis=0))[0:32] * scale

        wait_landed()
        near_sum = gathered(near, batches, 0)
        if last:
            own_sum[...] = gathered(own, owned, 0)
        wait_passed()
        at_batch = folded(near_sum + gathered(near, batches, 1), batches)
        if last:
            moments_out[...] = folded(own_sum[...] + gathered(own, owned, 1), owned)[0:harmonics]
        comp = lax.broadcasted_iota(jnp.int32, (32, LANES), 0)
        degree = sum((comp >= (l + 1) * (l + 1)).astype(F32) for l in range(4))
        damped = jnp.where(comp < harmonics, at_batch * (mixing_beta / (1.0 + degree)), 0.0)

        def density_step(step, ahead):
            for base in range(0, 16, SUBS // per_batch):
                parts = []
                for u in range(base, base + SUBS // per_batch):
                    col = jnp.broadcast_to(ahead[:, u : u + 1], (32, LANES))
                    for v in range(per_batch):
                        at = lane_tile((step * 16 + u) * per_batch + v)
                        part = col[24:32] * basis[24:25, at]
                        for g in range(3):
                            part = part + col[g * SUBS : (g + 1) * SUBS] * basis[g * SUBS : (g + 1) * SUBS, at]
                        parts.append(part)
                at = pl.multiple_of((step * 16 + base) * per_batch, SUBS)
                correct[pl.ds(at, SUBS), :] = stacked_sums(parts, sub)
            return pltpu.roll(ahead, LANES - 16, 1)

        lax.fori_loop(0, batches // 16, density_step, damped)
        density = base_rows[...] - correct[...]
        density_out[...] = density
        if not last:
            new = target[...] + coupling[...] * jnp.tanh(density) - density
            new_w = new * w[...]
            fresh[...] = new
            fresh_w[...] = new_w
            square = jnp.sum(new * new_w, axis=0, keepdims=True)


def finish(density, moments, density_out, moments_out, sem):
    copies = [
        pltpu.make_async_copy(density, density_out, sem.at[0]),
        pltpu.make_async_copy(moments, moments_out, sem.at[1]),
    ]
    for copy in copies:
        copy.start()
    for copy in copies:
        copy.wait()


def local(weights, target, coupling, multipole_basis, rho_hist, res_hist, batch_atom, owner_slot, slot_index):
    harmonics, points = multipole_basis.shape
    hist_len = res_hist.shape[0]
    batches = batch_atom.shape[0]
    groups = lax.axis_size("grid")
    members = lax.axis_size("atom")
    devices = groups * members
    owned = owner_slot.shape[0] // members
    scale = 1.0 / math.sqrt(points * groups // owned)
    iters = slot_index.shape[0]
    cfg = (iters, hist_len, harmonics, batches, points // batches, owned, groups, members, scale)
    tiles = points // LANES
    flat = (tiles, LANES)
    any_space = pl.BlockSpec(memory_space=pl.ANY)
    vmem = pl.BlockSpec(memory_space=pltpu.VMEM)
    density, moments = pl.pallas_call(
        functools.partial(kernel, cfg),
        out_shape=(jax.ShapeDtypeStruct(flat, F32), jax.ShapeDtypeStruct((harmonics, owned), F32)),
        in_specs=[any_space] * 9,
        out_specs=(vmem, vmem),
        scratch_shapes=[
            pltpu.VMEM(flat, F32),
            pltpu.VMEM(flat, F32),
            pltpu.VMEM(flat, F32),
            pltpu.VMEM((harmonics, points), F32),
            pltpu.VMEM((hist_len, points), F32),
            pltpu.VMEM((hist_len, points), F32),
            pltpu.VMEM(flat, F32),
            pltpu.VMEM(flat, F32),
            pltpu.VMEM((iters, devices, 1, LANES), F32),
            pltpu.VMEM((iters, batches // 4, LANES), F32),
            pltpu.VMEM((iters, 2, devices // 2, batches // 4, LANES), F32),
            pltpu.VMEM((4 * batches, devices * batches // 4), jnp.bfloat16),
            pltpu.VMEM((4 * owned, devices * batches // 4), jnp.bfloat16),
            pltpu.VMEM((owned, LANES), F32),
            pltpu.VMEM((batches // 4, SUBS, LANES), F32),
            pltpu.VMEM(flat, F32),
            pltpu.VMEM(flat, F32),
            pltpu.SMEM(batch_atom.shape, batch_atom.dtype),
            pltpu.SMEM(owner_slot.shape, owner_slot.dtype),
            pltpu.SMEM(slot_index.shape, slot_index.dtype),
            pltpu.SemaphoreType.DMA((9,)),
            pltpu.SemaphoreType.DMA((iters, 2)),
            pltpu.SemaphoreType.DMA((iters, 4, 2)),
        ],
        compiler_params=pltpu.CompilerParams(
            collective_id=0, has_side_effects=True, vmem_limit_bytes=40 * 1024 * 1024
        ),
    )(
        *(
            pltpu.with_memory_space_constraint(x, pltpu.HBM)
            for x in (
                batch_atom,
                owner_slot,
                slot_index,
                weights.reshape(flat),
                target.reshape(flat),
                coupling.reshape(flat),
                multipole_basis,
                rho_hist,
                res_hist,
            )
        )
    )
    density, moments = pl.pallas_call(
        finish,
        out_shape=(jax.ShapeDtypeStruct(flat, F32), jax.ShapeDtypeStruct((harmonics, owned), F32)),
        in_specs=[vmem] * 2,
        out_specs=(any_space, any_space),
        scratch_shapes=[pltpu.SemaphoreType.DMA((2,))],
    )(*(pltpu.with_memory_space_constraint(x, pltpu.VMEM) for x in (density, moments)))
    return density.reshape(points), moments


def solution(mesh):
    both = ("grid", "atom")
    placed = (P(both), P(both), P(both), P(None, both), P(None, both), P(None, both), P(both), P(), P())
    return jax.shard_map(
        local,
        mesh=mesh,
        in_specs=placed,
        out_specs=(P(both), P(None, "atom")),
        check_vma=False,
    )
```

```python
import functools
import math

import jax
import jax.numpy as jnp
from jax import lax
from jax.experimental import pallas as pl
from jax.experimental.pallas import tpu as pltpu
from jax.sharding import PartitionSpec as P

MESH = pl.DeviceIdType.MESH
LANES = 128
SUBS = 8
mixing_beta = 0.5
ridge_share = 0.1
F32 = jnp.float32


def solve_coeffs(entry, hist_len):
    trace = entry[0][0]
    for i in range(1, hist_len):
        trace = trace + entry[i][i]
    ridge = (ridge_share / hist_len) * trace
    low = [[entry[i][j] for j in range(i + 1)] for i in range(hist_len)]
    for i in range(hist_len):
        low[i][i] = low[i][i] + ridge
    inverse = [None] * hist_len
    factor = [[None] * hist_len for _ in range(hist_len)]
    forward = [jnp.ones_like(trace) for _ in range(hist_len)]
    for j in range(hist_len):
        inverse[j] = 1.0 / low[j][j]
        for i in range(j + 1, hist_len):
            factor[i][j] = low[i][j] * inverse[j]
        for i in range(j + 1, hist_len):
            forward[i] = forward[i] - factor[i][j] * forward[j]
            for k in range(j + 1, i + 1):
                low[i][k] = low[i][k] - factor[i][j] * low[k][j]
    backward = [forward[i] * inverse[i] for i in range(hist_len)]
    for j in reversed(range(hist_len)):
        for i in range(j):
            backward[i] = backward[i] - factor[j][i] * backward[j]
    total = backward[0]
    for i in range(1, hist_len):
        total = total + backward[i]
    return [backward[i] / total for i in range(hist_len)]


def split(x):
    pieces = []
    for _ in range(2):
        piece = x.astype(jnp.bfloat16).astype(F32)
        pieces.append(piece)
        x = x - piece
    return pieces


def flips(value, count):
    out = []
    bit = 1
    while bit < count:
        out.append(bit - 2 * bit * lax.rem(lax.div(value, bit), 2))
        bit *= 2
    return out


def flipped(value, changes, mask):
    for k, change in enumerate(changes):
        if mask >> k & 1:
            value = value + change
    return value


def kernel(
    cfg,
    batch_atom_hbm,
    owner_slot_hbm,
    slot_index_hbm,
    w_hbm,
    target_hbm,
    coupling_hbm,
    basis_hbm,
    rho_hbm,
    res_hbm,
    density_out,
    moments_out,
    w,
    target,
    coupling,
    basis,
    rho,
    res,
    fresh,
    fresh_w,
    row_bufs,
    sent_moments,
    all_moments,
    near,
    own,
    own_sum,
    halves,
    hist_moments,
    base_rows,
    correct,
    batch_atom,
    owner_slot,
    slot_index,
    load_sem,
    row_sem,
    moment_sem,
):
    iters, hist_len, harmonics, batches, width, owned, groups, members, scale = cfg
    devices = groups * members
    tiles = w.shape[0]
    per_batch = width // LANES
    half = LANES // 2
    rows = batches // 4
    my_group = lax.axis_index("grid")
    my_member = lax.axis_index("atom")
    me = my_group * members + my_member
    chips = devices // 2
    upper = chips // 2
    chip = lax.div(me, 2)
    core = lax.rem(me, 2)
    group_flips = flips(my_group, groups)
    member_flips = flips(my_member, members)

    def peer(step):
        return (
            flipped(my_group, group_flips, step // members),
            flipped(my_member, member_flips, step % members),
        )

    plane = min(chips, (members // 2) ** 2)
    chip_steps = [z * plane + p for p in reversed(range(plane)) for z in reversed(range(chips // plane))]
    device_steps = [2 * step + c for step in chip_steps for c in (1, 0)][:-1]

    barrier = pltpu.get_barrier_semaphore()

    loads = [
        pltpu.make_async_copy(src, dst, load_sem.at[k])
        for k, (src, dst) in enumerate(
            (
                (res_hbm, res),
                (w_hbm, w),
                (basis_hbm, basis),
                (rho_hbm, rho),
                (target_hbm, target),
                (coupling_hbm, coupling),
                (batch_atom_hbm, batch_atom),
                (owner_slot_hbm, owner_slot),
                (slot_index_hbm, slot_index),
            )
        )
    ]
    for k in (6, 7, 0, 1):
        loads[k].start()

    for step in device_steps:
        pl.semaphore_signal(barrier, inc=1, device_id=peer(step), device_id_type=MESH)

    for k in (2, 3, 4, 5, 8):
        loads[k].start()
    loads[6].wait()
    loads[7].wait()

    lane = lax.broadcasted_iota(jnp.int32, (SUBS, LANES), 1)
    sub = lax.broadcasted_iota(jnp.int32, (SUBS, LANES), 0)
    quarter = lane // 32
    lane_row = lax.broadcasted_iota(jnp.int32, (1, LANES), 1)

    slot_row = jnp.zeros((1, LANES), F32)
    slot_cols = []
    for block in range(batches // SUBS):
        col = jnp.zeros((SUBS, LANES), F32)
        for at in range(SUBS):
            b = block * SUBS + at
            slot = owner_slot[batch_atom[b]].astype(F32)
            slot_row = jnp.where(lane_row == half + b, slot, slot_row)
            col = jnp.where(sub == at, slot, col)
        slot_cols.append(col)
    slot_col = jnp.concatenate(slot_cols, axis=0)

    def lane_tile(t):
        return pl.ds(pl.multiple_of(t * LANES, LANES), LANES)

    def remote(src, dst, sems, step):
        return pltpu.make_async_remote_copy(
            src_ref=src,
            dst_ref=dst,
            send_sem=sems.at[0],
            recv_sem=sems.at[1],
            device_id=peer(step),
            device_id_type=MESH,
        )

    def exchange_rows(buf, sems):
        for step in device_steps:
            remote(buf.at[me], buf.at[me], sems, step).start()

        def wait():
            others = buf.at[pl.ds(0, devices - 1)]
            everyone = remote(others, others, sems, 1)
            everyone.wait_recv()
            everyone.wait_send()

        return wait

    def exchange_moments(mine, buf, sems):
        halves = [pl.ds((upper * k + chip - lax.rem(chip, upper)) % chips, upper) for k in range(2)]
        remote(mine, buf.at[0, chip], sems.at[0], 1).start()
        for step in chip_steps[:-1]:
            remote(mine, buf.at[0, chip], sems.at[step // upper], 2 * step + 1).start()
        landed = [remote(buf.at[0, half], buf.at[0, half], sems.at[k], 1) for k, half in enumerate(halves)]
        passed = [remote(buf.at[0, half], buf.at[1, half], sems.at[2 + k], 1) for k, half in enumerate(halves)]

        def wait_landed():
            for k in range(2):
                landed[k].wait_recv()
                passed[k].start()

        def wait_passed():
            for k in range(2):
                passed[k].wait_recv()
            for k in range(2):
                landed[k].wait_send()
                passed[k].wait_send()

        return wait_landed, wait_passed

    def total_row(buf):
        parts = [buf[spot] for spot in range(devices)]
        while len(parts) > 1:
            parts = [parts[k] + parts[k + 1] for k in range(0, len(parts), 2)]
        return parts[0]

    def splat(row, k):
        return jnp.broadcast_to(row[:, k : k + 1], (1, LANES))

    shifts = hist_len // 2 + 1
    entry = None
    for iteration in range(iters):
        row_buf = row_bufs.at[iteration]
        sent_buf = sent_moments.at[iteration]
        moment_buf = all_moments.at[iteration]
        last = iteration == iters - 1

        if iteration == 0:
            loads[0].wait()
            loads[1].wait()

            def gram(step, acc):
                acc = list(acc)
                for u in range(8):
                    t = step * 8 + u
                    x = res[:, lane_tile(t)]
                    y = x * w[pl.ds(t, 1), :]
                    for r in range(shifts):
                        acc[r] = acc[r] + y * (pltpu.roll(x, r, 0) if r else x)
                return tuple(acc)

            acc = lax.fori_loop(0, tiles // 8, gram, tuple(jnp.zeros((SUBS, LANES), F32) for _ in range(shifts)))
            packed = jnp.zeros((SUBS, LANES), F32)
            for r in range(shifts):
                packed = jnp.where(lane == hist_len * r + sub, jnp.sum(acc[r], axis=1, keepdims=True), packed)
            row_buf[pl.ds(me, 1)] = (jnp.sum(packed, axis=0, keepdims=True) + slot_row)[None]
            pl.semaphore_wait(barrier, devices - 1)
        else:
            slot = slot_index[iteration - 1]
            replaced = sub == slot

            acc = [jnp.zeros((SUBS, LANES), F32) for _ in range(4)]
            for t in range(tiles):
                acc[t % 4] = acc[t % 4] + fresh_w[t : t + 1, :] * res[:, t * LANES : (t + 1) * LANES]
            acc = (acc[0] + acc[1]) + (acc[2] + acc[3])
            acc = jnp.where(replaced, square, acc)
            packed = jnp.where(lane == sub, jnp.sum(acc, axis=1, keepdims=True), 0.0)
            row_buf[pl.ds(me, 1)] = jnp.sum(packed, axis=0, keepdims=True)[None]
        wait = exchange_rows(row_buf, row_sem.at[iteration])

        if iteration == 0:
            loads[2].wait()
        else:

            @pl.loop(0, tiles // 8)
            def _(step):
                for u in range(8):
                    t = step * 8 + u
                    res[:, lane_tile(t)] = jnp.where(replaced, fresh[pl.ds(t, 1), :], res[:, lane_tile(t)])
                    rho[:, lane_tile(t)] = jnp.where(replaced, density_out[pl.ds(t, 1), :], rho[:, lane_tile(t)])

        @pl.loop(0, rows)
        def _(r):
            xs, ys = [], []
            for q in range(4):
                b = q * rows + r
                at = pl.ds(pl.multiple_of(b * width, width), width)
                gain = jnp.concatenate([w[pl.ds(b * per_batch + v, 1), :] for v in range(per_batch)], axis=1)
                xs.extend(split(res[:, at] * gain))
                slab = pl.ds(pl.multiple_of(b * 32, 32), 32)
                if iteration == 0:
                    y = jnp.concatenate([basis[0:24, at], jnp.broadcast_to(basis[24:25, at], (SUBS, width))], axis=0)
                    pair = [piece.astype(jnp.bfloat16) for piece in split(y)]
                    for k in range(2):
                        halves[k, slab, :] = pair[k]
                else:
                    pair = [halves[k, slab, :] for k in range(2)]
                ys.append(pair)
            x = jnp.concatenate(xs, axis=0).astype(jnp.bfloat16)
            out = None
            for k in range(2):
                y = jnp.concatenate([pair[k] for pair in ys], axis=0)
                part = lax.dot_general(x, y, (((1,), (1,)), ((), ())), preferred_element_type=F32)
                out = part if out is None else out + part
            tile = jnp.zeros((SUBS, LANES), F32)
            for q in range(4):
                block = out[16 * q : 16 * q + 8] + out[16 * q + 8 : 16 * q + 16]
                tile = jnp.where(quarter == q, block, tile)
            hist_moments[r] = tile

        wait()

        row = total_row(row_buf)
        if iteration == 0:
            entry = [[None] * (i + 1) for i in range(hist_len)]
            for i in range(hist_len):
                for j in range(i + 1):
                    r = i - j
                    at = hist_len * r + i if r < shifts else hist_len * (hist_len - r) + j
                    entry[i][j] = splat(row, at)
        else:
            news = [splat(row, k) for k in range(hist_len)]
            slot_vec = jnp.zeros((1, LANES), jnp.int32) + slot
            entry = [
                [
                    jnp.where(slot_vec == i, news[j], jnp.where(slot_vec == j, news[i], entry[i][j]))
                    for j in range(i + 1)
                ]
                for i in range(hist_len)
            ]
        coeffs = solve_coeffs(entry, hist_len)
        coeff_col = jnp.zeros((SUBS, LANES), F32)
        for i in range(hist_len):
            coeff_col = jnp.where(sub == i, coeffs[i], coeff_col)

        mixed = [jnp.sum(coeff_col * hist_moments[r], axis=0, keepdims=True) for r in range(rows)]
        sent_buf[...] = jnp.concatenate(mixed, axis=0)
        wait_landed, wait_passed = exchange_moments(sent_buf, moment_buf, moment_sem.at[iteration])

        if iteration == 0:
            base = (my_member * owned).astype(F32)
            wide = lax.broadcasted_iota(jnp.int32, (owned, LANES), 0).astype(F32) + base

            @pl.loop(0, devices // SUBS)
            def _(c):
                side = lax.div(c, chips // SUBS)
                first = 2 * SUBS * lax.rem(c, chips // SUBS) + lax.rem(core + 1 + side, 2)
                ids = jnp.concatenate([row_buf[first + 2 * i] for i in range(SUBS)], axis=0)
                stepped = pltpu.roll(ids, 0, 1, stride=rows, stride_axis=0)
                for q in range(4):
                    turned = pltpu.roll(stepped, (half - rows * q) % LANES, 1)
                    slots = jnp.sum(jnp.where(lane // rows == sub, turned, 0.0), axis=0, keepdims=True)
                    near[q * batches : (q + 1) * batches, lane_tile(c)] = jnp.where(
                        slot_col == slots, 1.0, 0.0
                    ).astype(jnp.bfloat16)
                    own[q * owned : (q + 1) * owned, lane_tile(c)] = jnp.where(wide == slots, 1.0, 0.0).astype(
                        jnp.bfloat16
                    )

            for k in (3, 4, 5, 8):
                loads[k].wait()

        def base_step(step, carry):
            for u in range(8):
                t = step * 8 + u
                part = coeff_col * (rho[:, lane_tile(t)] + mixing_beta * res[:, lane_tile(t)])
                base_rows[pl.ds(t, 1), :] = jnp.sum(part, axis=0, keepdims=True)
            return carry

        lax.fori_loop(0, tiles // 8, base_step, 0)
        depth = chips * rows

        def gathered(mask, count, side):
            everywhere = moment_buf[side].reshape(depth, LANES)
            pieces = jnp.concatenate([piece.astype(jnp.bfloat16) for piece in split(everywhere)], axis=1)
            out = jnp.dot(mask[:, side * depth : (side + 1) * depth], pieces, preferred_element_type=F32)
            out = out[:, 0:LANES] + out[:, LANES:]
            group = lax.broadcasted_iota(jnp.int32, (count, LANES), 1) // 32
            total = out[0:count]
            for q in range(1, 4):
                total = jnp.where(group == q, out[q * count : (q + 1) * count], total)
            return total

        def folded(total):
            total = total + pltpu.roll(total, 64, 1)
            return (total + pltpu.roll(total, 32, 1)) * scale

        wait_landed()
        near_sum = gathered(near, batches, 0)
        if last:
            own_sum[...] = gathered(own, owned, 0)
        wait_passed()
        near_sum = near_sum + gathered(near, batches, 1)
        if last:
            own_sum[...] = own_sum[...] + gathered(own, owned, 1)
        at_batch = folded(near_sum)
        comp = lax.broadcasted_iota(jnp.int32, (batches, LANES), 1) % 32
        spot = lax.broadcasted_iota(jnp.int32, (batches, LANES), 0) % SUBS
        turn = lax.broadcasted_iota(jnp.int32, (batches, LANES), 1) // 32
        degree = sum((comp >= (l + 1) * (l + 1)).astype(F32) for l in range(4))
        damped = jnp.where(comp < harmonics, at_batch * (mixing_beta / (1.0 + degree)), 0.0)
        spread = jnp.concatenate([jnp.where(spot == turn + 4 * side, damped, 0.0) for side in range(2)], axis=1)
        high, low = split(spread)
        for g in range(batches // SUBS):
            mine = slice(g * SUBS, (g + 1) * SUBS)
            x = jnp.concatenate([high[mine], low[mine]], axis=0).astype(jnp.bfloat16)
            out = None
            for k in range(2):
                y = halves[k, g * SUBS * 32 : (g + 1) * SUBS * 32, :]
                part = jnp.dot(x, y, preferred_element_type=F32)
                out = part if out is None else out + part
            out = out[0:SUBS] + out[SUBS:]
            for v in range(per_batch):
                correct[pl.ds(g * SUBS * per_batch + v, SUBS, stride=per_batch), :] = out[
                    :, v * LANES : (v + 1) * LANES
                ]
        density = base_rows[...] - correct[...]
        density_out[...] = density
        if last:
            turned = jnp.transpose(own_sum[...])
            final = (turned[0:32] + turned[32:64]) + (turned[64:96] + turned[96:128])
            moments_out[...] = final[0:harmonics] * scale
        if not last:
            new = target[...] + coupling[...] * jnp.tanh(density) - density
            new_w = new * w[...]
            fresh[...] = new
            fresh_w[...] = new_w
            square = jnp.sum(new * new_w, axis=0, keepdims=True)


def finish(density, moments, density_out, moments_out, sem):
    copies = [
        pltpu.make_async_copy(density, density_out, sem.at[0]),
        pltpu.make_async_copy(moments, moments_out, sem.at[1]),
    ]
    for copy in copies:
        copy.start()
    for copy in copies:
        copy.wait()


def local(weights, target, coupling, multipole_basis, rho_hist, res_hist, batch_atom, owner_slot, slot_index):
    harmonics, points = multipole_basis.shape
    hist_len = res_hist.shape[0]
    batches = batch_atom.shape[0]
    groups = lax.axis_size("grid")
    members = lax.axis_size("atom")
    devices = groups * members
    owned = owner_slot.shape[0] // members
    scale = 1.0 / math.sqrt(points * groups // owned)
    iters = slot_index.shape[0]
    cfg = (iters, hist_len, harmonics, batches, points // batches, owned, groups, members, scale)
    tiles = points // LANES
    flat = (tiles, LANES)
    any_space = pl.BlockSpec(memory_space=pl.ANY)
    vmem = pl.BlockSpec(memory_space=pltpu.VMEM)
    density, moments = pl.pallas_call(
        functools.partial(kernel, cfg),
        out_shape=(jax.ShapeDtypeStruct(flat, F32), jax.ShapeDtypeStruct((harmonics, owned), F32)),
        in_specs=[any_space] * 9,
        out_specs=(vmem, vmem),
        scratch_shapes=[
            pltpu.VMEM(flat, F32),
            pltpu.VMEM(flat, F32),
            pltpu.VMEM(flat, F32),
            pltpu.VMEM((harmonics, points), F32),
            pltpu.VMEM((hist_len, points), F32),
            pltpu.VMEM((hist_len, points), F32),
            pltpu.VMEM(flat, F32),
            pltpu.VMEM(flat, F32),
            pltpu.VMEM((iters, devices, 1, LANES), F32),
            pltpu.VMEM((iters, batches // 4, LANES), F32),
            pltpu.VMEM((iters, 2, devices // 2, batches // 4, LANES), F32),
            pltpu.VMEM((4 * batches, devices * batches // 4), jnp.bfloat16),
            pltpu.VMEM((4 * owned, devices * batches // 4), jnp.bfloat16),
            pltpu.VMEM((owned, LANES), F32),
            pltpu.VMEM((2, batches * 32, points // batches), jnp.bfloat16),
            pltpu.VMEM((batches // 4, SUBS, LANES), F32),
            pltpu.VMEM(flat, F32),
            pltpu.VMEM(flat, F32),
            pltpu.SMEM(batch_atom.shape, batch_atom.dtype),
            pltpu.SMEM(owner_slot.shape, owner_slot.dtype),
            pltpu.SMEM(slot_index.shape, slot_index.dtype),
            pltpu.SemaphoreType.DMA((9,)),
            pltpu.SemaphoreType.DMA((iters, 2)),
            pltpu.SemaphoreType.DMA((iters, 4, 2)),
        ],
        compiler_params=pltpu.CompilerParams(
            collective_id=0, has_side_effects=True, vmem_limit_bytes=40 * 1024 * 1024
        ),
    )(
        *(
            pltpu.with_memory_space_constraint(x, pltpu.HBM)
            for x in (
                batch_atom,
                owner_slot,
                slot_index,
                weights.reshape(flat),
                target.reshape(flat),
                coupling.reshape(flat),
                multipole_basis,
                rho_hist,
                res_hist,
            )
        )
    )
    density, moments = pl.pallas_call(
        finish,
        out_shape=(jax.ShapeDtypeStruct(flat, F32), jax.ShapeDtypeStruct((harmonics, owned), F32)),
        in_specs=[vmem] * 2,
        out_specs=(any_space, any_space),
        scratch_shapes=[pltpu.SemaphoreType.DMA((2,))],
    )(*(pltpu.with_memory_space_constraint(x, pltpu.VMEM) for x in (density, moments)))
    return density.reshape(points), moments


def solution(mesh):
    both = ("grid", "atom")
    placed = (P(both), P(both), P(both), P(None, both), P(None, both), P(None, both), P(both), P(), P())
    return jax.shard_map(
        local,
        mesh=mesh,
        in_specs=placed,
        out_specs=(P(both), P(None, "atom")),
        check_vma=False,
    )
```

```python
import functools
import math

import jax
import jax.numpy as jnp
from jax import lax
from jax.experimental import pallas as pl
from jax.experimental.pallas import tpu as pltpu
from jax.sharding import PartitionSpec as P

MESH = pl.DeviceIdType.MESH
LANES = 128
SUBS = 8
mixing_beta = 0.5
ridge_share = 0.1
F32 = jnp.float32


def solve_coeffs(entry, hist_len):
    trace = entry[0][0]
    for i in range(1, hist_len):
        trace = trace + entry[i][i]
    ridge = (ridge_share / hist_len) * trace
    low = [[entry[i][j] for j in range(i + 1)] for i in range(hist_len)]
    for i in range(hist_len):
        low[i][i] = low[i][i] + ridge
    inverse = [None] * hist_len
    factor = [[None] * hist_len for _ in range(hist_len)]
    forward = [jnp.ones_like(trace) for _ in range(hist_len)]
    for j in range(hist_len):
        inverse[j] = 1.0 / low[j][j]
        for i in range(j + 1, hist_len):
            factor[i][j] = low[i][j] * inverse[j]
        for i in range(j + 1, hist_len):
            forward[i] = forward[i] - factor[i][j] * forward[j]
            for k in range(j + 1, i + 1):
                low[i][k] = low[i][k] - factor[i][j] * low[k][j]
    backward = [forward[i] * inverse[i] for i in range(hist_len)]
    for j in reversed(range(hist_len)):
        for i in range(j):
            backward[i] = backward[i] - factor[j][i] * backward[j]
    total = backward[0]
    for i in range(1, hist_len):
        total = total + backward[i]
    return [backward[i] / total for i in range(hist_len)]


def split(x):
    pieces = []
    for _ in range(2):
        piece = x.astype(jnp.bfloat16).astype(F32)
        pieces.append(piece)
        x = x - piece
    return pieces


def flips(value, count):
    out = []
    bit = 1
    while bit < count:
        out.append(bit - 2 * bit * lax.rem(lax.div(value, bit), 2))
        bit *= 2
    return out


def flipped(value, changes, mask):
    for k, change in enumerate(changes):
        if mask >> k & 1:
            value = value + change
    return value


def kernel(
    cfg,
    batch_atom_hbm,
    owner_slot_hbm,
    slot_index_hbm,
    w_hbm,
    target_hbm,
    coupling_hbm,
    basis_hbm,
    rho_hbm,
    res_hbm,
    density_out,
    moments_out,
    w,
    target,
    coupling,
    basis,
    rho,
    res,
    fresh,
    fresh_w,
    row_bufs,
    sent_moments,
    all_moments,
    near,
    own,
    own_sum,
    halves,
    hist_moments,
    base_rows,
    correct,
    batch_atom,
    owner_slot,
    slot_index,
    load_sem,
    row_sem,
    moment_sem,
):
    iters, hist_len, harmonics, batches, width, owned, groups, members, scale = cfg
    devices = groups * members
    tiles = w.shape[0]
    per_batch = width // LANES
    half = LANES // 2
    rows = batches // 4
    my_group = lax.axis_index("grid")
    my_member = lax.axis_index("atom")
    me = my_group * members + my_member
    chips = devices // 2
    upper = chips // 2
    chip = lax.div(me, 2)
    core = lax.rem(me, 2)
    group_flips = flips(my_group, groups)
    member_flips = flips(my_member, members)

    def peer(step):
        return (
            flipped(my_group, group_flips, step // members),
            flipped(my_member, member_flips, step % members),
        )

    plane = min(chips, (members // 2) ** 2)
    chip_steps = [z * plane + p for p in reversed(range(plane)) for z in reversed(range(chips // plane))]
    device_steps = [2 * step + c for step in chip_steps for c in (1, 0)][:-1]

    barrier = pltpu.get_barrier_semaphore()

    loads = [
        pltpu.make_async_copy(src, dst, load_sem.at[k])
        for k, (src, dst) in enumerate(
            (
                (res_hbm, res),
                (w_hbm, w),
                (basis_hbm, basis),
                (rho_hbm, rho),
                (target_hbm, target),
                (coupling_hbm, coupling),
                (batch_atom_hbm, batch_atom),
                (owner_slot_hbm, owner_slot),
                (slot_index_hbm, slot_index),
            )
        )
    ]
    for k in (6, 7, 0, 1):
        loads[k].start()

    for step in device_steps:
        pl.semaphore_signal(barrier, inc=1, device_id=peer(step), device_id_type=MESH)

    for k in (2, 3, 4, 5, 8):
        loads[k].start()
    loads[6].wait()
    loads[7].wait()

    lane = lax.broadcasted_iota(jnp.int32, (SUBS, LANES), 1)
    sub = lax.broadcasted_iota(jnp.int32, (SUBS, LANES), 0)
    quarter = lane // 32
    lane_row = lax.broadcasted_iota(jnp.int32, (1, LANES), 1)

    slot_row = jnp.zeros((1, LANES), F32)
    slot_cols = []
    for block in range(batches // SUBS):
        col = jnp.zeros((SUBS, LANES), F32)
        for at in range(SUBS):
            b = block * SUBS + at
            slot = owner_slot[batch_atom[b]].astype(F32)
            slot_row = jnp.where(lane_row == half + b, slot, slot_row)
            col = jnp.where(sub == at, slot, col)
        slot_cols.append(col)
    slot_col = jnp.concatenate(slot_cols, axis=0)

    def lane_tile(t):
        return pl.ds(pl.multiple_of(t * LANES, LANES), LANES)

    def remote(src, dst, sems, step):
        return pltpu.make_async_remote_copy(
            src_ref=src,
            dst_ref=dst,
            send_sem=sems.at[0],
            recv_sem=sems.at[1],
            device_id=peer(step),
            device_id_type=MESH,
        )

    def exchange_rows(buf, sems):
        for step in device_steps:
            remote(buf.at[me], buf.at[me], sems, step).start()

        def wait():
            others = buf.at[pl.ds(0, devices - 1)]
            everyone = remote(others, others, sems, 1)
            everyone.wait_recv()
            everyone.wait_send()

        return wait

    def exchange_moments(mine, buf, sems, favour):
        halves = [pl.ds((upper * k + chip - lax.rem(chip, upper)) % chips, upper) for k in range(2)]
        remote(mine, buf.at[0, chip], sems.at[0], 1).start()
        def send(step):
            remote(mine, buf.at[0, chip], sems.at[step // upper], 2 * step + 1).start()

        if favour:
            origin = pltpu.make_async_remote_copy(
                src_ref=mine,
                dst_ref=buf.at[0, chip],
                send_sem=sems.at[lax.div(chip, upper), 0],
                recv_sem=sems.at[lax.div(chip, upper), 1],
                device_id=(0, 1 - core),
                device_id_type=MESH,
            )
            pl.when(chip != 0)(origin.start)
            for step in chip_steps[:-1]:
                pl.when(chip != step)(functools.partial(send, step))
        else:
            for step in chip_steps[:-1]:
                send(step)
        landed = [remote(buf.at[0, half], buf.at[0, half], sems.at[k], 1) for k, half in enumerate(halves)]
        passed = [remote(buf.at[0, half], buf.at[1, half], sems.at[2 + k], 1) for k, half in enumerate(halves)]

        def wait_landed():
            for k in range(2):
                landed[k].wait_recv()
                passed[k].start()

        def wait_passed():
            for k in range(2):
                passed[k].wait_recv()
            for k in range(2):
                landed[k].wait_send()
                passed[k].wait_send()

        return wait_landed, wait_passed

    def total_row(buf):
        parts = [buf[spot] for spot in range(devices)]
        while len(parts) > 1:
            parts = [parts[k] + parts[k + 1] for k in range(0, len(parts), 2)]
        return parts[0]

    def splat(row, k):
        return jnp.broadcast_to(row[:, k : k + 1], (1, LANES))

    shifts = hist_len // 2 + 1
    entry = None
    for iteration in range(iters):
        row_buf = row_bufs.at[iteration]
        sent_buf = sent_moments.at[iteration]
        moment_buf = all_moments.at[iteration]
        last = iteration == iters - 1

        if iteration == 0:
            loads[0].wait()
            loads[1].wait()

            def gram(step, acc):
                acc = list(acc)
                for u in range(8):
                    t = step * 8 + u
                    x = res[:, lane_tile(t)]
                    y = x * w[pl.ds(t, 1), :]
                    for r in range(shifts):
                        acc[r] = acc[r] + y * (pltpu.roll(x, r, 0) if r else x)
                return tuple(acc)

            acc = lax.fori_loop(0, tiles // 8, gram, tuple(jnp.zeros((SUBS, LANES), F32) for _ in range(shifts)))
            packed = jnp.zeros((SUBS, LANES), F32)
            for r in range(shifts):
                packed = jnp.where(lane == hist_len * r + sub, jnp.sum(acc[r], axis=1, keepdims=True), packed)
            row_buf[pl.ds(me, 1)] = (jnp.sum(packed, axis=0, keepdims=True) + slot_row)[None]
            pl.semaphore_wait(barrier, devices - 1)
        else:
            slot = slot_index[iteration - 1]
            replaced = sub == slot

            acc = [jnp.zeros((SUBS, LANES), F32) for _ in range(4)]
            for t in range(tiles):
                acc[t % 4] = acc[t % 4] + fresh_w[t : t + 1, :] * res[:, t * LANES : (t + 1) * LANES]
            acc = (acc[0] + acc[1]) + (acc[2] + acc[3])
            acc = jnp.where(replaced, square, acc)
            packed = jnp.where(lane == sub, jnp.sum(acc, axis=1, keepdims=True), 0.0)
            row_buf[pl.ds(me, 1)] = jnp.sum(packed, axis=0, keepdims=True)[None]
        wait = exchange_rows(row_buf, row_sem.at[iteration])

        if iteration == 0:
            loads[2].wait()
        else:

            @pl.loop(0, tiles // 8)
            def _(step):
                for u in range(8):
                    t = step * 8 + u
                    res[:, lane_tile(t)] = jnp.where(replaced, fresh[pl.ds(t, 1), :], res[:, lane_tile(t)])
                    rho[:, lane_tile(t)] = jnp.where(replaced, density_out[pl.ds(t, 1), :], rho[:, lane_tile(t)])

        @pl.loop(0, rows)
        def _(r):
            xs, ys = [], []
            for q in range(4):
                b = q * rows + r
                at = pl.ds(pl.multiple_of(b * width, width), width)
                gain = jnp.concatenate([w[pl.ds(b * per_batch + v, 1), :] for v in range(per_batch)], axis=1)
                xs.extend(split(res[:, at] * gain))
                slab = pl.ds(pl.multiple_of(b * 32, 32), 32)
                if iteration == 0:
                    y = jnp.concatenate([basis[0:24, at], jnp.broadcast_to(basis[24:25, at], (SUBS, width))], axis=0)
                    pair = [piece.astype(jnp.bfloat16) for piece in split(y)]
                    for k in range(2):
                        halves[k, slab, :] = pair[k]
                else:
                    pair = [halves[k, slab, :] for k in range(2)]
                ys.append(pair)
            x = jnp.concatenate(xs, axis=0).astype(jnp.bfloat16)
            out = None
            for k in range(2):
                y = jnp.concatenate([pair[k] for pair in ys], axis=0)
                part = lax.dot_general(x, y, (((1,), (1,)), ((), ())), preferred_element_type=F32)
                out = part if out is None else out + part
            tile = jnp.zeros((SUBS, LANES), F32)
            for q in range(4):
                block = out[16 * q : 16 * q + 8] + out[16 * q + 8 : 16 * q + 16]
                tile = jnp.where(quarter == q, block, tile)
            hist_moments[r] = tile

        wait()

        row = total_row(row_buf)
        if iteration == 0:
            entry = [[None] * (i + 1) for i in range(hist_len)]
            for i in range(hist_len):
                for j in range(i + 1):
                    r = i - j
                    at = hist_len * r + i if r < shifts else hist_len * (hist_len - r) + j
                    entry[i][j] = splat(row, at)
        else:
            news = [splat(row, k) for k in range(hist_len)]
            slot_vec = jnp.zeros((1, LANES), jnp.int32) + slot
            entry = [
                [
                    jnp.where(slot_vec == i, news[j], jnp.where(slot_vec == j, news[i], entry[i][j]))
                    for j in range(i + 1)
                ]
                for i in range(hist_len)
            ]
        coeffs = solve_coeffs(entry, hist_len)
        coeff_col = jnp.zeros((SUBS, LANES), F32)
        for i in range(hist_len):
            coeff_col = jnp.where(sub == i, coeffs[i], coeff_col)

        mixed = [jnp.sum(coeff_col * hist_moments[r], axis=0, keepdims=True) for r in range(rows)]
        sent_buf[...] = jnp.concatenate(mixed, axis=0)
        wait_landed, wait_passed = exchange_moments(sent_buf, moment_buf, moment_sem.at[iteration], last)

        if iteration == 0:
            base = (my_member * owned).astype(F32)
            wide = lax.broadcasted_iota(jnp.int32, (owned, LANES), 0).astype(F32) + base

            @pl.loop(0, devices // SUBS)
            def _(c):
                side = lax.div(c, chips // SUBS)
                first = 2 * SUBS * lax.rem(c, chips // SUBS) + lax.rem(core + 1 + side, 2)
                ids = jnp.concatenate([row_buf[first + 2 * i] for i in range(SUBS)], axis=0)
                stepped = pltpu.roll(ids, 0, 1, stride=rows, stride_axis=0)
                for q in range(4):
                    turned = pltpu.roll(stepped, (half - rows * q) % LANES, 1)
                    slots = jnp.sum(jnp.where(lane // rows == sub, turned, 0.0), axis=0, keepdims=True)
                    near[q * batches : (q + 1) * batches, lane_tile(c)] = jnp.where(
                        slot_col == slots, 1.0, 0.0
                    ).astype(jnp.bfloat16)
                    own[:, lane_tile(4 * c + q)] = jnp.where(wide == slots, 1.0, 0.0).astype(jnp.bfloat16)

            for k in (3, 4, 5, 8):
                loads[k].wait()

        def base_step(step, carry):
            for u in range(8):
                t = step * 8 + u
                part = coeff_col * (rho[:, lane_tile(t)] + mixing_beta * res[:, lane_tile(t)])
                base_rows[pl.ds(t, 1), :] = jnp.sum(part, axis=0, keepdims=True)
            return carry

        lax.fori_loop(0, tiles // 8, base_step, 0)
        depth = chips * rows

        def pieces_of(side):
            everywhere = moment_buf[side].reshape(depth, LANES)
            return jnp.concatenate([piece.astype(jnp.bfloat16) for piece in split(everywhere)], axis=1)

        def near_part(pieces, side):
            out = jnp.dot(near[:, side * depth : (side + 1) * depth], pieces, preferred_element_type=F32)
            out = out[:, 0:LANES] + out[:, LANES:]
            group = lax.broadcasted_iota(jnp.int32, (batches, LANES), 1) // 32
            total = out[0:batches]
            for q in range(1, 4):
                total = jnp.where(group == q, out[q * batches : (q + 1) * batches], total)
            return total

        def own_part(pieces, side):
            turn = lax.broadcasted_iota(jnp.int32, (1, 2 * LANES), 1) % LANES // 32
            picks = [jnp.where(turn == q, 1.0, 0.0).astype(jnp.bfloat16) for q in range(4)]
            stacked = jnp.concatenate(
                [pieces[c : c + LANES] * pick for c in range(0, depth, LANES) for pick in picks], axis=0
            )
            outs = []
            for k in range(2):
                mine = own[k * owned // 2 : (k + 1) * owned // 2, 4 * side * depth : 4 * (side + 1) * depth]
                out = jnp.dot(mine, stacked, preferred_element_type=F32)
                outs.append(out[:, 0:LANES] + out[:, LANES:])
            return jnp.concatenate(outs, axis=0)

        def folded(total):
            total = total + pltpu.roll(total, 64, 1)
            return (total + pltpu.roll(total, 32, 1)) * scale

        wait_landed()
        pieces = pieces_of(0)
        near_sum = near_part(pieces, 0)
        if last:
            own_sum[...] = own_part(pieces, 0)
        wait_passed()
        pieces = pieces_of(1)
        near_sum = near_sum + near_part(pieces, 1)
        if last:
            own_sum[...] = own_sum[...] + own_part(pieces, 1)
        at_batch = folded(near_sum)
        comp = lax.broadcasted_iota(jnp.int32, (batches, LANES), 1) % 32
        spot = lax.broadcasted_iota(jnp.int32, (batches, LANES), 0) % SUBS
        turn = lax.broadcasted_iota(jnp.int32, (batches, LANES), 1) // 32
        degree = sum((comp >= (l + 1) * (l + 1)).astype(F32) for l in range(4))
        damped = jnp.where(comp < harmonics, at_batch * (mixing_beta / (1.0 + degree)), 0.0)
        spread = jnp.concatenate([jnp.where(spot == turn + 4 * side, damped, 0.0) for side in range(2)], axis=1)
        high, low = split(spread)
        for g in range(batches // SUBS):
            mine = slice(g * SUBS, (g + 1) * SUBS)
            x = jnp.concatenate([high[mine], low[mine]], axis=0).astype(jnp.bfloat16)
            out = None
            for k in range(2):
                y = halves[k, g * SUBS * 32 : (g + 1) * SUBS * 32, :]
                part = jnp.dot(x, y, preferred_element_type=F32)
                out = part if out is None else out + part
            out = out[0:SUBS] + out[SUBS:]
            for v in range(per_batch):
                correct[pl.ds(g * SUBS * per_batch + v, SUBS, stride=per_batch), :] = out[
                    :, v * LANES : (v + 1) * LANES
                ]
        density = base_rows[...] - correct[...]
        density_out[...] = density
        if last:
            turned = jnp.transpose(own_sum[...])
            final = (turned[0:32] + turned[32:64]) + (turned[64:96] + turned[96:128])
            moments_out[...] = final[0:harmonics] * scale
        if not last:
            new = target[...] + coupling[...] * jnp.tanh(density) - density
            new_w = new * w[...]
            fresh[...] = new
            fresh_w[...] = new_w
            square = jnp.sum(new * new_w, axis=0, keepdims=True)


def finish(density, moments, density_out, moments_out, sem):
    copies = [
        pltpu.make_async_copy(density, density_out, sem.at[0]),
        pltpu.make_async_copy(moments, moments_out, sem.at[1]),
    ]
    for copy in copies:
        copy.start()
    for copy in copies:
        copy.wait()


def local(weights, target, coupling, multipole_basis, rho_hist, res_hist, batch_atom, owner_slot, slot_index):
    harmonics, points = multipole_basis.shape
    hist_len = res_hist.shape[0]
    batches = batch_atom.shape[0]
    groups = lax.axis_size("grid")
    members = lax.axis_size("atom")
    devices = groups * members
    owned = owner_slot.shape[0] // members
    scale = 1.0 / math.sqrt(points * groups // owned)
    iters = slot_index.shape[0]
    cfg = (iters, hist_len, harmonics, batches, points // batches, owned, groups, members, scale)
    tiles = points // LANES
    flat = (tiles, LANES)
    any_space = pl.BlockSpec(memory_space=pl.ANY)
    vmem = pl.BlockSpec(memory_space=pltpu.VMEM)
    density, moments = pl.pallas_call(
        functools.partial(kernel, cfg),
        out_shape=(jax.ShapeDtypeStruct(flat, F32), jax.ShapeDtypeStruct((harmonics, owned), F32)),
        in_specs=[any_space] * 9,
        out_specs=(vmem, vmem),
        scratch_shapes=[
            pltpu.VMEM(flat, F32),
            pltpu.VMEM(flat, F32),
            pltpu.VMEM(flat, F32),
            pltpu.VMEM((harmonics, points), F32),
            pltpu.VMEM((hist_len, points), F32),
            pltpu.VMEM((hist_len, points), F32),
            pltpu.VMEM(flat, F32),
            pltpu.VMEM(flat, F32),
            pltpu.VMEM((iters, devices, 1, LANES), F32),
            pltpu.VMEM((iters, batches // 4, LANES), F32),
            pltpu.VMEM((iters, 2, devices // 2, batches // 4, LANES), F32),
            pltpu.VMEM((4 * batches, devices * batches // 4), jnp.bfloat16),
            pltpu.VMEM((owned, devices * batches), jnp.bfloat16),
            pltpu.VMEM((owned, LANES), F32),
            pltpu.VMEM((2, batches * 32, points // batches), jnp.bfloat16),
            pltpu.VMEM((batches // 4, SUBS, LANES), F32),
            pltpu.VMEM(flat, F32),
            pltpu.VMEM(flat, F32),
            pltpu.SMEM(batch_atom.shape, batch_atom.dtype),
            pltpu.SMEM(owner_slot.shape, owner_slot.dtype),
            pltpu.SMEM(slot_index.shape, slot_index.dtype),
            pltpu.SemaphoreType.DMA((9,)),
            pltpu.SemaphoreType.DMA((iters, 2)),
            pltpu.SemaphoreType.DMA((iters, 4, 2)),
        ],
        compiler_params=pltpu.CompilerParams(
            collective_id=0, has_side_effects=True, vmem_limit_bytes=40 * 1024 * 1024
        ),
    )(
        *(
            pltpu.with_memory_space_constraint(x, pltpu.HBM)
            for x in (
                batch_atom,
                owner_slot,
                slot_index,
                weights.reshape(flat),
                target.reshape(flat),
                coupling.reshape(flat),
                multipole_basis,
                rho_hist,
                res_hist,
            )
        )
    )
    density, moments = pl.pallas_call(
        finish,
        out_shape=(jax.ShapeDtypeStruct(flat, F32), jax.ShapeDtypeStruct((harmonics, owned), F32)),
        in_specs=[vmem] * 2,
        out_specs=(any_space, any_space),
        scratch_shapes=[pltpu.SemaphoreType.DMA((2,))],
    )(*(pltpu.with_memory_space_constraint(x, pltpu.VMEM) for x in (density, moments)))
    return density.reshape(points), moments


def solution(mesh):
    both = ("grid", "atom")
    placed = (P(both), P(both), P(both), P(None, both), P(None, both), P(None, both), P(both), P(), P())
    return jax.shard_map(
        local,
        mesh=mesh,
        in_specs=placed,
        out_specs=(P(both), P(None, "atom")),
        check_vma=False,
    )
```

```python
import functools
import math

import jax
import jax.numpy as jnp
from jax import lax
from jax.experimental import pallas as pl
from jax.experimental.pallas import tpu as pltpu
from jax.sharding import PartitionSpec as P

MESH = pl.DeviceIdType.MESH
LANES = 128
SUBS = 8
mixing_beta = 0.5
ridge_share = 0.1
F32 = jnp.float32


def solve_coeffs(entry, hist_len):
    trace = entry[0][0]
    for i in range(1, hist_len):
        trace = trace + entry[i][i]
    ridge = (ridge_share / hist_len) * trace
    low = [[entry[i][j] for j in range(i + 1)] for i in range(hist_len)]
    for i in range(hist_len):
        low[i][i] = low[i][i] + ridge
    inverse = [None] * hist_len
    factor = [[None] * hist_len for _ in range(hist_len)]
    forward = [jnp.ones_like(trace) for _ in range(hist_len)]
    for j in range(hist_len):
        inverse[j] = 1.0 / low[j][j]
        for i in range(j + 1, hist_len):
            factor[i][j] = low[i][j] * inverse[j]
        for i in range(j + 1, hist_len):
            forward[i] = forward[i] - factor[i][j] * forward[j]
            for k in range(j + 1, i + 1):
                low[i][k] = low[i][k] - factor[i][j] * low[k][j]
    backward = [forward[i] * inverse[i] for i in range(hist_len)]
    for j in reversed(range(hist_len)):
        for i in range(j):
            backward[i] = backward[i] - factor[j][i] * backward[j]
    total = backward[0]
    for i in range(1, hist_len):
        total = total + backward[i]
    return [backward[i] / total for i in range(hist_len)]


def split(x):
    pieces = []
    for _ in range(2):
        piece = x.astype(jnp.bfloat16).astype(F32)
        pieces.append(piece)
        x = x - piece
    return pieces


def flips(value, count):
    out = []
    bit = 1
    while bit < count:
        out.append(bit - 2 * bit * lax.rem(lax.div(value, bit), 2))
        bit *= 2
    return out


def flipped(value, changes, mask):
    for k, change in enumerate(changes):
        if mask >> k & 1:
            value = value + change
    return value


def kernel(
    cfg,
    batch_atom_hbm,
    owner_slot_hbm,
    slot_index_hbm,
    w_hbm,
    target_hbm,
    coupling_hbm,
    basis_hbm,
    rho_hbm,
    res_hbm,
    density_out,
    moments_out,
    w,
    target,
    coupling,
    basis,
    rho,
    res,
    fresh,
    row_bufs,
    sent_moments,
    all_moments,
    near,
    own,
    own_sum,
    halves,
    hist_moments,
    base_rows,
    batch_atom,
    owner_slot,
    slot_index,
    load_sem,
    row_sem,
    moment_sem,
):
    iters, hist_len, harmonics, batches, width, owned, groups, members, scale = cfg
    devices = groups * members
    tiles = w.shape[0]
    per_batch = width // LANES
    half = LANES // 2
    rows = batches // 4
    my_group = lax.axis_index("grid")
    my_member = lax.axis_index("atom")
    me = my_group * members + my_member
    chips = devices // 2
    upper = chips // 2
    chip = lax.div(me, 2)
    core = lax.rem(me, 2)
    group_flips = flips(my_group, groups)
    member_flips = flips(my_member, members)

    def peer(step):
        return (
            flipped(my_group, group_flips, step // members),
            flipped(my_member, member_flips, step % members),
        )

    plane = min(chips, (members // 2) ** 2)
    chip_steps = [z * plane + p for p in reversed(range(plane)) for z in reversed(range(chips // plane))]
    device_steps = [2 * step + c for c in (0, 1) for step in chip_steps]
    device_steps.remove(0)

    barrier = pltpu.get_barrier_semaphore()

    loads = [
        pltpu.make_async_copy(src, dst, load_sem.at[k])
        for k, (src, dst) in enumerate(
            (
                (res_hbm, res),
                (w_hbm, w),
                (basis_hbm, basis),
                (rho_hbm, rho),
                (target_hbm, target),
                (coupling_hbm, coupling),
                (batch_atom_hbm, batch_atom),
                (owner_slot_hbm, owner_slot),
                (slot_index_hbm, slot_index),
            )
        )
    ]
    for k in (6, 7, 0, 1):
        loads[k].start()

    for step in device_steps:
        pl.semaphore_signal(barrier, inc=1, device_id=peer(step), device_id_type=MESH)

    for k in (2, 3, 4, 5, 8):
        loads[k].start()
    loads[6].wait()
    loads[7].wait()

    lane = lax.broadcasted_iota(jnp.int32, (SUBS, LANES), 1)
    sub = lax.broadcasted_iota(jnp.int32, (SUBS, LANES), 0)
    quarter = lane // 32
    lane_row = lax.broadcasted_iota(jnp.int32, (1, LANES), 1)

    slot_row = jnp.zeros((1, LANES), F32)
    slot_cols = []
    for block in range(batches // SUBS):
        col = jnp.zeros((SUBS, LANES), F32)
        for at in range(SUBS):
            b = block * SUBS + at
            slot = owner_slot[batch_atom[b]].astype(F32)
            slot_row = jnp.where(lane_row == half + b, slot, slot_row)
            col = jnp.where(sub == at, slot, col)
        slot_cols.append(col)
    slot_col = jnp.concatenate(slot_cols, axis=0)

    def lane_tile(t):
        return pl.ds(pl.multiple_of(t * LANES, LANES), LANES)

    def remote(src, dst, sems, step):
        return pltpu.make_async_remote_copy(
            src_ref=src,
            dst_ref=dst,
            send_sem=sems.at[0],
            recv_sem=sems.at[1],
            device_id=peer(step),
            device_id_type=MESH,
        )

    def exchange_rows(buf, sems):
        for step in device_steps:
            remote(buf.at[me], buf.at[me], sems, step).start()

        def wait():
            others = buf.at[pl.ds(0, devices - 1)]
            everyone = remote(others, others, sems, 1)
            everyone.wait_recv()
            everyone.wait_send()

        return wait

    def exchange_moments(mine, buf, sems, favour):
        halves = [pl.ds((upper * k + chip - lax.rem(chip, upper)) % chips, upper) for k in range(2)]
        remote(mine, buf.at[0, chip], sems.at[0], 1).start()
        def send(step):
            remote(mine, buf.at[0, chip], sems.at[step // upper], 2 * step + 1).start()

        if favour:
            origin = pltpu.make_async_remote_copy(
                src_ref=mine,
                dst_ref=buf.at[0, chip],
                send_sem=sems.at[lax.div(chip, upper), 0],
                recv_sem=sems.at[lax.div(chip, upper), 1],
                device_id=(0, 1 - core),
                device_id_type=MESH,
            )
            pl.when(chip != 0)(origin.start)
            for step in chip_steps[:-1]:
                pl.when(chip != step)(functools.partial(send, step))
        else:
            for step in chip_steps[:-1]:
                send(step)
        landed = [remote(buf.at[0, half], buf.at[0, half], sems.at[k], 1) for k, half in enumerate(halves)]
        passed = [remote(buf.at[0, half], buf.at[1, half], sems.at[2 + k], 1) for k, half in enumerate(halves)]

        def wait_landed():
            for k in range(2):
                landed[k].wait_recv()
                passed[k].start()

        def wait_passed():
            for k in range(2):
                passed[k].wait_recv()
            for k in range(2):
                landed[k].wait_send()
                passed[k].wait_send()

        return wait_landed, wait_passed

    def total_row(buf):
        parts = [buf[spot] for spot in range(devices)]
        while len(parts) > 1:
            parts = [parts[k] + parts[k + 1] for k in range(0, len(parts), 2)]
        return parts[0]

    def splat(row, k):
        return jnp.broadcast_to(row[:, k : k + 1], (1, LANES))

    shifts = hist_len // 2 + 1
    entry = None
    for iteration in range(iters):
        row_buf = row_bufs.at[iteration]
        sent_buf = sent_moments.at[iteration]
        moment_buf = all_moments.at[iteration]
        last = iteration == iters - 1

        if iteration == 0:
            loads[0].wait()
            loads[1].wait()

            def gram(step, acc):
                acc = list(acc)
                for u in range(8):
                    t = step * 8 + u
                    x = res[:, lane_tile(t)]
                    y = x * w[pl.ds(t, 1), :]
                    for r in range(shifts):
                        acc[r] = acc[r] + y * (pltpu.roll(x, r, 0) if r else x)
                return tuple(acc)

            acc = lax.fori_loop(0, tiles // 8, gram, tuple(jnp.zeros((SUBS, LANES), F32) for _ in range(shifts)))
            packed = jnp.zeros((SUBS, LANES), F32)
            for r in range(shifts):
                packed = jnp.where(lane == hist_len * r + sub, jnp.sum(acc[r], axis=1, keepdims=True), packed)
            row_buf[pl.ds(me, 1)] = (jnp.sum(packed, axis=0, keepdims=True) + slot_row)[None]
            pl.semaphore_wait(barrier, devices - 1)
        else:
            slot = slot_index[iteration - 1]
            replaced = sub == slot

            acc = (acc[0] + acc[1]) + (acc[2] + acc[3])
            square = jnp.sum(square, axis=0, keepdims=True)
            acc = jnp.where(replaced, square, acc)
            packed = jnp.where(lane == sub, jnp.sum(acc, axis=1, keepdims=True), 0.0)
            row_buf[pl.ds(me, 1)] = jnp.sum(packed, axis=0, keepdims=True)[None]
        wait = exchange_rows(row_buf, row_sem.at[iteration])

        if iteration == 0:
            loads[2].wait()
        else:

            @pl.loop(0, tiles // 8)
            def _(step):
                for u in range(8):
                    t = step * 8 + u
                    res[:, lane_tile(t)] = jnp.where(replaced, fresh[pl.ds(t, 1), :], res[:, lane_tile(t)])
                    rho[:, lane_tile(t)] = jnp.where(replaced, density_out[pl.ds(t, 1), :], rho[:, lane_tile(t)])

        @pl.loop(0, rows)
        def _(r):
            xs, ys = [], []
            for q in range(4):
                b = q * rows + r
                at = pl.ds(pl.multiple_of(b * width, width), width)
                gain = jnp.concatenate([w[pl.ds(b * per_batch + v, 1), :] for v in range(per_batch)], axis=1)
                xs.extend(split(res[:, at] * gain))
                slab = pl.ds(pl.multiple_of(b * 32, 32), 32)
                if iteration == 0:
                    y = jnp.concatenate([basis[0:24, at], jnp.broadcast_to(basis[24:25, at], (SUBS, width))], axis=0)
                    pair = [piece.astype(jnp.bfloat16) for piece in split(y)]
                    for k in range(2):
                        halves[k, slab, :] = pair[k]
                else:
                    pair = [halves[k, slab, :] for k in range(2)]
                ys.append(pair)
            x = jnp.concatenate(xs, axis=0).astype(jnp.bfloat16)
            out = None
            for k in range(2):
                y = jnp.concatenate([pair[k] for pair in ys], axis=0)
                part = lax.dot_general(x, y, (((1,), (1,)), ((), ())), preferred_element_type=F32)
                out = part if out is None else out + part
            tile = jnp.zeros((SUBS, LANES), F32)
            for q in range(4):
                block = out[16 * q : 16 * q + 8] + out[16 * q + 8 : 16 * q + 16]
                tile = jnp.where(quarter == q, block, tile)
            hist_moments[r] = tile

        wait()

        row = total_row(row_buf)
        if iteration == 0:
            entry = [[None] * (i + 1) for i in range(hist_len)]
            for i in range(hist_len):
                for j in range(i + 1):
                    r = i - j
                    at = hist_len * r + i if r < shifts else hist_len * (hist_len - r) + j
                    entry[i][j] = splat(row, at)
        else:
            news = [splat(row, k) for k in range(hist_len)]
            slot_vec = jnp.zeros((1, LANES), jnp.int32) + slot
            entry = [
                [
                    jnp.where(slot_vec == i, news[j], jnp.where(slot_vec == j, news[i], entry[i][j]))
                    for j in range(i + 1)
                ]
                for i in range(hist_len)
            ]
        coeffs = solve_coeffs(entry, hist_len)
        coeff_col = jnp.zeros((SUBS, LANES), F32)
        for i in range(hist_len):
            coeff_col = jnp.where(sub == i, coeffs[i], coeff_col)

        mixed = [jnp.sum(coeff_col * hist_moments[r], axis=0, keepdims=True) for r in range(rows)]
        sent_buf[...] = jnp.concatenate(mixed, axis=0)
        wait_landed, wait_passed = exchange_moments(sent_buf, moment_buf, moment_sem.at[iteration], last)

        if iteration == 0:
            base = (my_member * owned).astype(F32)
            wide = lax.broadcasted_iota(jnp.int32, (owned, LANES), 0).astype(F32) + base

            @pl.loop(0, devices // SUBS)
            def _(c):
                side = lax.div(c, chips // SUBS)
                first = 2 * SUBS * lax.rem(c, chips // SUBS) + lax.rem(core + 1 + side, 2)
                ids = jnp.concatenate([row_buf[first + 2 * i] for i in range(SUBS)], axis=0)
                stepped = pltpu.roll(ids, 0, 1, stride=rows, stride_axis=0)
                for q in range(4):
                    turned = pltpu.roll(stepped, (half - rows * q) % LANES, 1)
                    slots = jnp.sum(jnp.where(lane // rows == sub, turned, 0.0), axis=0, keepdims=True)
                    near[q * batches : (q + 1) * batches, lane_tile(c)] = jnp.where(
                        slot_col == slots, 1.0, 0.0
                    ).astype(jnp.bfloat16)
                    own[:, lane_tile(4 * c + q)] = jnp.where(wide == slots, 1.0, 0.0).astype(jnp.bfloat16)

            for k in (3, 4, 5, 8):
                loads[k].wait()

        def base_step(step, carry):
            for u in range(8):
                t = step * 8 + u
                part = coeff_col * (rho[:, lane_tile(t)] + mixing_beta * res[:, lane_tile(t)])
                base_rows[pl.ds(t, 1), :] = jnp.sum(part, axis=0, keepdims=True)
            return carry

        lax.fori_loop(0, tiles // 8, base_step, 0)
        depth = chips * rows

        def pieces_of(side):
            everywhere = moment_buf[side].reshape(depth, LANES)
            return jnp.concatenate([piece.astype(jnp.bfloat16) for piece in split(everywhere)], axis=1)

        def near_part(pieces, side):
            out = jnp.dot(near[:, side * depth : (side + 1) * depth], pieces, preferred_element_type=F32)
            out = out[:, 0:LANES] + out[:, LANES:]
            group = lax.broadcasted_iota(jnp.int32, (batches, LANES), 1) // 32
            total = out[0:batches]
            for q in range(1, 4):
                total = jnp.where(group == q, out[q * batches : (q + 1) * batches], total)
            return total

        def own_part(pieces, side):
            turn = lax.broadcasted_iota(jnp.int32, (1, 2 * LANES), 1) % LANES // 32
            picks = [jnp.where(turn == q, 1.0, 0.0).astype(jnp.bfloat16) for q in range(4)]
            stacked = jnp.concatenate(
                [pieces[c : c + LANES] * pick for c in range(0, depth, LANES) for pick in picks], axis=0
            )
            outs = []
            for k in range(2):
                mine = own[k * owned // 2 : (k + 1) * owned // 2, 4 * side * depth : 4 * (side + 1) * depth]
                out = jnp.dot(mine, stacked, preferred_element_type=F32)
                outs.append(out[:, 0:LANES] + out[:, LANES:])
            return jnp.concatenate(outs, axis=0)

        def folded(total):
            total = total + pltpu.roll(total, 64, 1)
            return (total + pltpu.roll(total, 32, 1)) * scale

        wait_landed()
        pieces = pieces_of(0)
        near_sum = near_part(pieces, 0)
        if last:
            own_sum[...] = own_part(pieces, 0)
        wait_passed()
        pieces = pieces_of(1)
        near_sum = near_sum + near_part(pieces, 1)
        if last:
            own_sum[...] = own_sum[...] + own_part(pieces, 1)
        at_batch = folded(near_sum)
        comp = lax.broadcasted_iota(jnp.int32, (batches, LANES), 1) % 32
        spot = lax.broadcasted_iota(jnp.int32, (batches, LANES), 0) % SUBS
        turn = lax.broadcasted_iota(jnp.int32, (batches, LANES), 1) // 32
        degree = sum((comp >= (l + 1) * (l + 1)).astype(F32) for l in range(4))
        damped = jnp.where(comp < harmonics, at_batch * (mixing_beta / (1.0 + degree)), 0.0)
        spread = jnp.concatenate([jnp.where(spot == turn + 4 * side, damped, 0.0) for side in range(2)], axis=1)
        high, low = split(spread)
        acc = [jnp.zeros((SUBS, LANES), F32) for _ in range(4)]
        square = jnp.zeros((SUBS, LANES), F32)
        for g in range(batches // SUBS):
            mine = slice(g * SUBS, (g + 1) * SUBS)
            x = jnp.concatenate([high[mine], low[mine]], axis=0).astype(jnp.bfloat16)
            out = None
            for k in range(2):
                y = halves[k, g * SUBS * 32 : (g + 1) * SUBS * 32, :]
                part = jnp.dot(x, y, preferred_element_type=F32)
                out = part if out is None else out + part
            out = out[0:SUBS] + out[SUBS:]
            for v in range(per_batch):
                lines = pl.ds(g * SUBS * per_batch + v, SUBS, stride=per_batch)
                density = base_rows[lines, :] - out[:, v * LANES : (v + 1) * LANES]
                density_out[lines, :] = density
                if not last:
                    new = target[lines, :] + coupling[lines, :] * jnp.tanh(density) - density
                    new_w = new * w[lines, :]
                    fresh[lines, :] = new
                    square = square + new * new_w
                    for k in range(SUBS):
                        t = (g * SUBS + k) * per_batch + v
                        line = jnp.broadcast_to(new_w[k : k + 1, :], (SUBS, LANES))
                        acc[k % 4] = acc[k % 4] + line * res[:, t * LANES : (t + 1) * LANES]
        if last:
            turned = jnp.transpose(own_sum[...])
            final = (turned[0:32] + turned[32:64]) + (turned[64:96] + turned[96:128])
            moments_out[...] = final[0:harmonics] * scale


def finish(density, moments, density_out, moments_out, sem):
    copies = [
        pltpu.make_async_copy(density, density_out, sem.at[0]),
        pltpu.make_async_copy(moments, moments_out, sem.at[1]),
    ]
    for copy in copies:
        copy.start()
    for copy in copies:
        copy.wait()


def local(weights, target, coupling, multipole_basis, rho_hist, res_hist, batch_atom, owner_slot, slot_index):
    harmonics, points = multipole_basis.shape
    hist_len = res_hist.shape[0]
    batches = batch_atom.shape[0]
    groups = lax.axis_size("grid")
    members = lax.axis_size("atom")
    devices = groups * members
    owned = owner_slot.shape[0] // members
    scale = 1.0 / math.sqrt(points * groups // owned)
    iters = slot_index.shape[0]
    cfg = (iters, hist_len, harmonics, batches, points // batches, owned, groups, members, scale)
    tiles = points // LANES
    flat = (tiles, LANES)
    any_space = pl.BlockSpec(memory_space=pl.ANY)
    vmem = pl.BlockSpec(memory_space=pltpu.VMEM)
    density, moments = pl.pallas_call(
        functools.partial(kernel, cfg),
        out_shape=(jax.ShapeDtypeStruct(flat, F32), jax.ShapeDtypeStruct((harmonics, owned), F32)),
        in_specs=[any_space] * 9,
        out_specs=(vmem, vmem),
        scratch_shapes=[
            pltpu.VMEM(flat, F32),
            pltpu.VMEM(flat, F32),
            pltpu.VMEM(flat, F32),
            pltpu.VMEM((harmonics, points), F32),
            pltpu.VMEM((hist_len, points), F32),
            pltpu.VMEM((hist_len, points), F32),
            pltpu.VMEM(flat, F32),
            pltpu.VMEM((iters, devices, 1, LANES), F32),
            pltpu.VMEM((iters, batches // 4, LANES), F32),
            pltpu.VMEM((iters, 2, devices // 2, batches // 4, LANES), F32),
            pltpu.VMEM((4 * batches, devices * batches // 4), jnp.bfloat16),
            pltpu.VMEM((owned, devices * batches), jnp.bfloat16),
            pltpu.VMEM((owned, LANES), F32),
            pltpu.VMEM((2, batches * 32, points // batches), jnp.bfloat16),
            pltpu.VMEM((batches // 4, SUBS, LANES), F32),
            pltpu.VMEM(flat, F32),
            pltpu.SMEM(batch_atom.shape, batch_atom.dtype),
            pltpu.SMEM(owner_slot.shape, owner_slot.dtype),
            pltpu.SMEM(slot_index.shape, slot_index.dtype),
            pltpu.SemaphoreType.DMA((9,)),
            pltpu.SemaphoreType.DMA((iters, 2)),
            pltpu.SemaphoreType.DMA((iters, 4, 2)),
        ],
        compiler_params=pltpu.CompilerParams(
            collective_id=0, has_side_effects=True, vmem_limit_bytes=40 * 1024 * 1024
        ),
    )(
        *(
            pltpu.with_memory_space_constraint(x, pltpu.HBM)
            for x in (
                batch_atom,
                owner_slot,
                slot_index,
                weights.reshape(flat),
                target.reshape(flat),
                coupling.reshape(flat),
                multipole_basis,
                rho_hist,
                res_hist,
            )
        )
    )
    density, moments = pl.pallas_call(
        finish,
        out_shape=(jax.ShapeDtypeStruct(flat, F32), jax.ShapeDtypeStruct((harmonics, owned), F32)),
        in_specs=[vmem] * 2,
        out_specs=(any_space, any_space),
        scratch_shapes=[pltpu.SemaphoreType.DMA((2,))],
    )(*(pltpu.with_memory_space_constraint(x, pltpu.VMEM) for x in (density, moments)))
    return density.reshape(points), moments


def solution(mesh):
    both = ("grid", "atom")
    placed = (P(both), P(both), P(both), P(None, both), P(None, both), P(None, both), P(both), P(), P())
    return jax.shard_map(
        local,
        mesh=mesh,
        in_specs=placed,
        out_specs=(P(both), P(None, "atom")),
        check_vma=False,
    )
```

```python
import functools
import math

import jax
import jax.numpy as jnp
from jax import lax
from jax.experimental import pallas as pl
from jax.experimental.pallas import tpu as pltpu
from jax.sharding import PartitionSpec as P

MESH = pl.DeviceIdType.MESH
LANES = 128
SUBS = 8
mixing_beta = 0.5
ridge_share = 0.1
F32 = jnp.float32


def solve_coeffs(entry, hist_len):
    trace = entry[0][0]
    for i in range(1, hist_len):
        trace = trace + entry[i][i]
    ridge = (ridge_share / hist_len) * trace
    low = [[entry[i][j] for j in range(i + 1)] for i in range(hist_len)]
    for i in range(hist_len):
        low[i][i] = low[i][i] + ridge
    inverse = [None] * hist_len
    factor = [[None] * hist_len for _ in range(hist_len)]
    forward = [jnp.ones_like(trace) for _ in range(hist_len)]
    for j in range(hist_len):
        inverse[j] = 1.0 / low[j][j]
        for i in range(j + 1, hist_len):
            factor[i][j] = low[i][j] * inverse[j]
        for i in range(j + 1, hist_len):
            forward[i] = forward[i] - factor[i][j] * forward[j]
            for k in range(j + 1, i + 1):
                low[i][k] = low[i][k] - factor[i][j] * low[k][j]
    backward = [forward[i] * inverse[i] for i in range(hist_len)]
    for j in reversed(range(hist_len)):
        for i in range(j):
            backward[i] = backward[i] - factor[j][i] * backward[j]
    total = backward[0]
    for i in range(1, hist_len):
        total = total + backward[i]
    return [backward[i] / total for i in range(hist_len)]


def split(x):
    pieces = []
    for _ in range(2):
        piece = x.astype(jnp.bfloat16).astype(F32)
        pieces.append(piece)
        x = x - piece
    return pieces


def flips(value, count):
    out = []
    bit = 1
    while bit < count:
        out.append(bit - 2 * bit * lax.rem(lax.div(value, bit), 2))
        bit *= 2
    return out


def flipped(value, changes, mask):
    for k, change in enumerate(changes):
        if mask >> k & 1:
            value = value + change
    return value


def kernel(
    cfg,
    batch_atom_hbm,
    owner_slot_hbm,
    slot_index_hbm,
    w_hbm,
    target_hbm,
    coupling_hbm,
    basis_hbm,
    rho_hbm,
    res_hbm,
    density_out,
    moments_out,
    w,
    target,
    coupling,
    basis,
    rho,
    res,
    fresh,
    row_bufs,
    sent_moments,
    all_moments,
    near,
    own,
    own_sum,
    halves,
    hist_moments,
    base_rows,
    batch_atom,
    owner_slot,
    slot_index,
    load_sem,
    row_sem,
    moment_sem,
):
    iters, hist_len, harmonics, batches, width, owned, groups, members, scale = cfg
    devices = groups * members
    tiles = w.shape[0]
    per_batch = width // LANES
    half = LANES // 2
    rows = batches // 4
    my_group = lax.axis_index("grid")
    my_member = lax.axis_index("atom")
    me = my_group * members + my_member
    chips = devices // 2
    upper = chips // 2
    chip = lax.div(me, 2)
    core = lax.rem(me, 2)
    group_flips = flips(my_group, groups)
    member_flips = flips(my_member, members)

    def peer(step):
        return (
            flipped(my_group, group_flips, step // members),
            flipped(my_member, member_flips, step % members),
        )

    plane = min(chips, (members // 2) ** 2)
    chip_steps = [z * plane + p for p in reversed(range(plane)) for z in reversed(range(chips // plane))]
    device_steps = [2 * step + c for c in (0, 1) for step in chip_steps]
    device_steps.remove(0)

    barrier = pltpu.get_barrier_semaphore()

    loads = [
        pltpu.make_async_copy(src, dst, load_sem.at[k])
        for k, (src, dst) in enumerate(
            (
                (res_hbm, res),
                (w_hbm, w),
                (basis_hbm, basis),
                (rho_hbm, rho),
                (target_hbm, target),
                (coupling_hbm, coupling),
                (batch_atom_hbm, batch_atom),
                (owner_slot_hbm, owner_slot),
                (slot_index_hbm, slot_index),
            )
        )
    ]
    for k in (6, 7, 0, 1):
        loads[k].start()

    for step in device_steps:
        pl.semaphore_signal(barrier, inc=1, device_id=peer(step), device_id_type=MESH)

    for k in (2, 3, 4, 5, 8):
        loads[k].start()
    loads[6].wait()
    loads[7].wait()

    lane = lax.broadcasted_iota(jnp.int32, (SUBS, LANES), 1)
    sub = lax.broadcasted_iota(jnp.int32, (SUBS, LANES), 0)
    quarter = lane // 32
    lane_row = lax.broadcasted_iota(jnp.int32, (1, LANES), 1)

    slot_row = jnp.zeros((1, LANES), F32)
    slot_cols = []
    for block in range(batches // SUBS):
        col = jnp.zeros((SUBS, LANES), F32)
        for at in range(SUBS):
            b = block * SUBS + at
            slot = owner_slot[batch_atom[b]].astype(F32)
            slot_row = jnp.where(lane_row == half + b, slot, slot_row)
            col = jnp.where(sub == at, slot, col)
        slot_cols.append(col)
    slot_col = jnp.concatenate(slot_cols, axis=0)

    def lane_tile(t):
        return pl.ds(pl.multiple_of(t * LANES, LANES), LANES)

    def remote(src, dst, sems, step):
        return pltpu.make_async_remote_copy(
            src_ref=src,
            dst_ref=dst,
            send_sem=sems.at[0],
            recv_sem=sems.at[1],
            device_id=peer(step),
            device_id_type=MESH,
        )

    def exchange_rows(buf, sems):
        for step in device_steps:
            remote(buf.at[me], buf.at[me], sems, step).start()

        def wait():
            others = buf.at[pl.ds(0, devices - 1)]
            everyone = remote(others, others, sems, 1)
            everyone.wait_recv()
            everyone.wait_send()

        return wait

    def exchange_moments(mine, buf, sems, favour):
        halves = [pl.ds((upper * k + chip - lax.rem(chip, upper)) % chips, upper) for k in range(2)]
        remote(mine, buf.at[0, chip], sems.at[0], 1).start()
        def send(step):
            remote(mine, buf.at[0, chip], sems.at[step // upper], 2 * step + 1).start()

        if favour:
            origin = pltpu.make_async_remote_copy(
                src_ref=mine,
                dst_ref=buf.at[0, chip],
                send_sem=sems.at[lax.div(chip, upper), 0],
                recv_sem=sems.at[lax.div(chip, upper), 1],
                device_id=(0, 1 - core),
                device_id_type=MESH,
            )
            pl.when(chip != 0)(origin.start)
            for step in chip_steps[:-1]:
                pl.when(chip != step)(functools.partial(send, step))
        else:
            for step in chip_steps[:-1]:
                send(step)
        landed = [remote(buf.at[0, half], buf.at[0, half], sems.at[k], 1) for k, half in enumerate(halves)]
        passed = [remote(buf.at[0, half], buf.at[1, half], sems.at[2 + k], 1) for k, half in enumerate(halves)]

        def wait_landed():
            for k in range(2):
                landed[k].wait_recv()
                passed[k].start()

        def wait_passed():
            for k in range(2):
                passed[k].wait_recv()
            for k in range(2):
                landed[k].wait_send()
                passed[k].wait_send()

        return wait_landed, wait_passed

    def total_row(buf):
        parts = [buf[spot] for spot in range(devices)]
        while len(parts) > 1:
            parts = [parts[k] + parts[k + 1] for k in range(0, len(parts), 2)]
        return parts[0]

    def splat(row, k):
        return jnp.broadcast_to(row[:, k : k + 1], (1, LANES))

    shifts = hist_len // 2 + 1
    entry = None
    for iteration in range(iters):
        row_buf = row_bufs.at[iteration]
        sent_buf = sent_moments.at[iteration]
        moment_buf = all_moments.at[iteration]
        last = iteration == iters - 1

        if iteration == 0:
            loads[0].wait()
            loads[1].wait()

            def gram(step, acc):
                acc = list(acc)
                for u in range(8):
                    t = step * 8 + u
                    x = res[:, lane_tile(t)]
                    y = x * w[pl.ds(t, 1), :]
                    for r in range(shifts):
                        acc[r] = acc[r] + y * (pltpu.roll(x, r, 0) if r else x)
                return tuple(acc)

            acc = lax.fori_loop(0, tiles // 8, gram, tuple(jnp.zeros((SUBS, LANES), F32) for _ in range(shifts)))
            packed = jnp.zeros((SUBS, LANES), F32)
            for r in range(shifts):
                packed = jnp.where(lane == hist_len * r + sub, jnp.sum(acc[r], axis=1, keepdims=True), packed)
            row_buf[pl.ds(me, 1)] = (jnp.sum(packed, axis=0, keepdims=True) + slot_row)[None]
            pl.semaphore_wait(barrier, devices - 1)
        else:
            slot = slot_index[iteration - 1]
            replaced = sub == slot

            acc = (acc[0] + acc[1]) + (acc[2] + acc[3])
            square = jnp.sum(square, axis=0, keepdims=True)
            acc = jnp.where(replaced, square, acc)
            packed = jnp.where(lane == sub, jnp.sum(acc, axis=1, keepdims=True), 0.0)
            row_buf[pl.ds(me, 1)] = jnp.sum(packed, axis=0, keepdims=True)[None]
        wait = exchange_rows(row_buf, row_sem)

        if iteration == 0:
            loads[2].wait()
        else:

            @pl.loop(0, tiles // 8)
            def _(step):
                for u in range(8):
                    t = step * 8 + u
                    res[:, lane_tile(t)] = jnp.where(replaced, fresh[pl.ds(t, 1), :], res[:, lane_tile(t)])
                    rho[:, lane_tile(t)] = jnp.where(replaced, density_out[pl.ds(t, 1), :], rho[:, lane_tile(t)])

        @pl.loop(0, rows)
        def _(r):
            xs, ys = [], []
            for q in range(4):
                b = q * rows + r
                at = pl.ds(pl.multiple_of(b * width, width), width)
                gain = jnp.concatenate([w[pl.ds(b * per_batch + v, 1), :] for v in range(per_batch)], axis=1)
                xs.extend(split(res[:, at] * gain))
                slab = pl.ds(pl.multiple_of(b * 32, 32), 32)
                if iteration == 0:
                    y = jnp.concatenate([basis[0:24, at], jnp.broadcast_to(basis[24:25, at], (SUBS, width))], axis=0)
                    pair = [piece.astype(jnp.bfloat16) for piece in split(y)]
                    for k in range(2):
                        halves[k, slab, :] = pair[k]
                else:
                    pair = [halves[k, slab, :] for k in range(2)]
                ys.append(pair)
            x = jnp.concatenate(xs, axis=0).astype(jnp.bfloat16)
            out = None
            for k in range(2):
                y = jnp.concatenate([pair[k] for pair in ys], axis=0)
                part = lax.dot_general(x, y, (((1,), (1,)), ((), ())), preferred_element_type=F32)
                out = part if out is None else out + part
            tile = jnp.zeros((SUBS, LANES), F32)
            for q in range(4):
                block = out[16 * q : 16 * q + 8] + out[16 * q + 8 : 16 * q + 16]
                tile = jnp.where(quarter == q, block, tile)
            hist_moments[r] = tile

        wait()

        row = total_row(row_buf)
        if iteration == 0:
            entry = [[None] * (i + 1) for i in range(hist_len)]
            for i in range(hist_len):
                for j in range(i + 1):
                    r = i - j
                    at = hist_len * r + i if r < shifts else hist_len * (hist_len - r) + j
                    entry[i][j] = splat(row, at)
        else:
            news = [splat(row, k) for k in range(hist_len)]
            slot_vec = jnp.zeros((1, LANES), jnp.int32) + slot
            entry = [
                [
                    jnp.where(slot_vec == i, news[j], jnp.where(slot_vec == j, news[i], entry[i][j]))
                    for j in range(i + 1)
                ]
                for i in range(hist_len)
            ]
        coeffs = solve_coeffs(entry, hist_len)
        coeff_col = jnp.zeros((SUBS, LANES), F32)
        for i in range(hist_len):
            coeff_col = jnp.where(sub == i, coeffs[i], coeff_col)

        mixed = [jnp.sum(coeff_col * hist_moments[r], axis=0, keepdims=True) for r in range(rows)]
        sent_buf[...] = jnp.concatenate(mixed, axis=0)
        wait_landed, wait_passed = exchange_moments(sent_buf, moment_buf, moment_sem, last)

        if iteration == 0:
            base = (my_member * owned).astype(F32)
            wide = lax.broadcasted_iota(jnp.int32, (owned, LANES), 0).astype(F32) + base

            @pl.loop(0, devices // SUBS)
            def _(c):
                side = lax.div(c, chips // SUBS)
                first = 2 * SUBS * lax.rem(c, chips // SUBS) + lax.rem(core + 1 + side, 2)
                ids = jnp.concatenate([row_buf[first + 2 * i] for i in range(SUBS)], axis=0)
                stepped = pltpu.roll(ids, 0, 1, stride=rows, stride_axis=0)
                for q in range(4):
                    turned = pltpu.roll(stepped, (half - rows * q) % LANES, 1)
                    slots = jnp.sum(jnp.where(lane // rows == sub, turned, 0.0), axis=0, keepdims=True)
                    near[q * batches : (q + 1) * batches, lane_tile(c)] = jnp.where(
                        slot_col == slots, 1.0, 0.0
                    ).astype(jnp.bfloat16)
                    own[:, lane_tile(4 * c + q)] = jnp.where(wide == slots, 1.0, 0.0).astype(jnp.bfloat16)

            for k in (3, 4, 5, 8):
                loads[k].wait()

        def base_step(step, carry):
            for u in range(8):
                t = step * 8 + u
                part = coeff_col * (rho[:, lane_tile(t)] + mixing_beta * res[:, lane_tile(t)])
                base_rows[pl.ds(t, 1), :] = jnp.sum(part, axis=0, keepdims=True)
            return carry

        lax.fori_loop(0, tiles // 8, base_step, 0)
        depth = chips * rows

        def pieces_of(side):
            everywhere = moment_buf[side].reshape(depth, LANES)
            return jnp.concatenate([piece.astype(jnp.bfloat16) for piece in split(everywhere)], axis=1)

        def near_part(pieces, side):
            group = lax.broadcasted_iota(jnp.int32, (batches, LANES), 1) // 32
            total = None
            for half in range(2):
                lines = slice(2 * half * batches, 2 * (half + 1) * batches)
                out = jnp.dot(near[lines, side * depth : (side + 1) * depth], pieces, preferred_element_type=F32)
                out = out[:, 0:LANES] + out[:, LANES:]
                pair = jnp.where(group % 2 == 0, out[0:batches], out[batches:])
                total = pair if half == 0 else jnp.where(group // 2 == 0, total, pair)
            return total

        def own_part(pieces, side):
            turn = lax.broadcasted_iota(jnp.int32, (1, 2 * LANES), 1) % LANES // 32
            picks = [jnp.where(turn == q, 1.0, 0.0).astype(jnp.bfloat16) for q in range(4)]
            stacked = jnp.concatenate(
                [pieces[c : c + LANES] * pick for c in range(0, depth, LANES) for pick in picks], axis=0
            )
            outs = []
            for k in range(2):
                mine = own[k * owned // 2 : (k + 1) * owned // 2, 4 * side * depth : 4 * (side + 1) * depth]
                out = jnp.dot(mine, stacked, preferred_element_type=F32)
                outs.append(out[:, 0:LANES] + out[:, LANES:])
            return jnp.concatenate(outs, axis=0)

        def folded(total):
            total = total + pltpu.roll(total, 64, 1)
            return (total + pltpu.roll(total, 32, 1)) * scale

        wait_landed()
        pieces = pieces_of(0)
        near_sum = near_part(pieces, 0)
        if last:
            own_sum[...] = own_part(pieces, 0)
        wait_passed()
        pieces = pieces_of(1)
        near_sum = near_sum + near_part(pieces, 1)
        if last:
            own_sum[...] = own_sum[...] + own_part(pieces, 1)
        at_batch = folded(near_sum)
        comp = lax.broadcasted_iota(jnp.int32, (batches, LANES), 1) % 32
        spot = lax.broadcasted_iota(jnp.int32, (batches, LANES), 0) % SUBS
        turn = lax.broadcasted_iota(jnp.int32, (batches, LANES), 1) // 32
        degree = sum((comp >= (l + 1) * (l + 1)).astype(F32) for l in range(4))
        damped = jnp.where(comp < harmonics, at_batch * (mixing_beta / (1.0 + degree)), 0.0)
        spread = jnp.concatenate([jnp.where(spot == turn + 4 * side, damped, 0.0) for side in range(2)], axis=1)
        high, low = split(spread)
        acc = [jnp.zeros((SUBS, LANES), F32) for _ in range(4)]
        square = jnp.zeros((SUBS, LANES), F32)
        for g in range(batches // SUBS):
            mine = slice(g * SUBS, (g + 1) * SUBS)
            x = jnp.concatenate([high[mine], low[mine]], axis=0).astype(jnp.bfloat16)
            out = None
            for k in range(2):
                y = halves[k, g * SUBS * 32 : (g + 1) * SUBS * 32, :]
                part = jnp.dot(x, y, preferred_element_type=F32)
                out = part if out is None else out + part
            out = out[0:SUBS] + out[SUBS:]
            for v in range(per_batch):
                lines = pl.ds(g * SUBS * per_batch + v, SUBS, stride=per_batch)
                density = base_rows[lines, :] - out[:, v * LANES : (v + 1) * LANES]
                density_out[lines, :] = density
                if not last:
                    new = target[lines, :] + coupling[lines, :] * jnp.tanh(density) - density
                    new_w = new * w[lines, :]
                    fresh[lines, :] = new
                    square = square + new * new_w
                    for k in range(SUBS):
                        t = (g * SUBS + k) * per_batch + v
                        line = jnp.broadcast_to(new_w[k : k + 1, :], (SUBS, LANES))
                        acc[k % 4] = acc[k % 4] + line * res[:, t * LANES : (t + 1) * LANES]
        if last:
            turned = jnp.transpose(own_sum[...])
            final = (turned[0:32] + turned[32:64]) + (turned[64:96] + turned[96:128])
            moments_out[...] = final[0:harmonics] * scale


def finish(density, moments, density_out, moments_out, sem):
    copies = [
        pltpu.make_async_copy(density, density_out, sem.at[0]),
        pltpu.make_async_copy(moments, moments_out, sem.at[1]),
    ]
    for copy in copies:
        copy.start()
    for copy in copies:
        copy.wait()


def local(weights, target, coupling, multipole_basis, rho_hist, res_hist, batch_atom, owner_slot, slot_index):
    harmonics, points = multipole_basis.shape
    hist_len = res_hist.shape[0]
    batches = batch_atom.shape[0]
    groups = lax.axis_size("grid")
    members = lax.axis_size("atom")
    devices = groups * members
    owned = owner_slot.shape[0] // members
    scale = 1.0 / math.sqrt(points * groups // owned)
    iters = slot_index.shape[0]
    cfg = (iters, hist_len, harmonics, batches, points // batches, owned, groups, members, scale)
    tiles = points // LANES
    flat = (tiles, LANES)
    any_space = pl.BlockSpec(memory_space=pl.ANY)
    vmem = pl.BlockSpec(memory_space=pltpu.VMEM)
    density, moments = pl.pallas_call(
        functools.partial(kernel, cfg),
        out_shape=(jax.ShapeDtypeStruct(flat, F32), jax.ShapeDtypeStruct((harmonics, owned), F32)),
        in_specs=[any_space] * 9,
        out_specs=(vmem, vmem),
        scratch_shapes=[
            pltpu.VMEM(flat, F32),
            pltpu.VMEM(flat, F32),
            pltpu.VMEM(flat, F32),
            pltpu.VMEM((harmonics, points), F32),
            pltpu.VMEM((hist_len, points), F32),
            pltpu.VMEM((hist_len, points), F32),
            pltpu.VMEM(flat, F32),
            pltpu.VMEM((iters, devices, 1, LANES), F32),
            pltpu.VMEM((iters, batches // 4, LANES), F32),
            pltpu.VMEM((iters, 2, devices // 2, batches // 4, LANES), F32),
            pltpu.VMEM((4 * batches, devices * batches // 4), jnp.bfloat16),
            pltpu.VMEM((owned, devices * batches), jnp.bfloat16),
            pltpu.VMEM((owned, LANES), F32),
            pltpu.VMEM((2, batches * 32, points // batches), jnp.bfloat16),
            pltpu.VMEM((batches // 4, SUBS, LANES), F32),
            pltpu.VMEM(flat, F32),
            pltpu.SMEM(batch_atom.shape, batch_atom.dtype),
            pltpu.SMEM(owner_slot.shape, owner_slot.dtype),
            pltpu.SMEM(slot_index.shape, slot_index.dtype),
            pltpu.SemaphoreType.DMA((9,)),
            pltpu.SemaphoreType.DMA((2,)),
            pltpu.SemaphoreType.DMA((4, 2)),
        ],
        compiler_params=pltpu.CompilerParams(
            collective_id=0, has_side_effects=True, vmem_limit_bytes=40 * 1024 * 1024
        ),
    )(
        *(
            pltpu.with_memory_space_constraint(x, pltpu.HBM)
            for x in (
                batch_atom,
                owner_slot,
                slot_index,
                weights.reshape(flat),
                target.reshape(flat),
                coupling.reshape(flat),
                multipole_basis,
                rho_hist,
                res_hist,
            )
        )
    )
    density, moments = pl.pallas_call(
        finish,
        out_shape=(jax.ShapeDtypeStruct(flat, F32), jax.ShapeDtypeStruct((harmonics, owned), F32)),
        in_specs=[vmem] * 2,
        out_specs=(any_space, any_space),
        scratch_shapes=[pltpu.SemaphoreType.DMA((2,))],
    )(*(pltpu.with_memory_space_constraint(x, pltpu.VMEM) for x in (density, moments)))
    return density.reshape(points), moments


def solution(mesh):
    both = ("grid", "atom")
    placed = (P(both), P(both), P(both), P(None, both), P(None, both), P(None, both), P(both), P(), P())
    return jax.shard_map(
        local,
        mesh=mesh,
        in_specs=placed,
        out_specs=(P(both), P(None, "atom")),
        check_vma=False,
    )
```

```python
import functools
import math

import jax
import jax.numpy as jnp
from jax import lax
from jax.experimental import pallas as pl
from jax.experimental.pallas import tpu as pltpu
from jax.sharding import PartitionSpec as P

MESH = pl.DeviceIdType.MESH
LANES = 128
SUBS = 8
mixing_beta = 0.5
ridge_share = 0.1
F32 = jnp.float32


def solve_coeffs(entry, hist_len):
    trace = entry[0][0]
    for i in range(1, hist_len):
        trace = trace + entry[i][i]
    ridge = (ridge_share / hist_len) * trace
    low = [[entry[i][j] for j in range(i + 1)] for i in range(hist_len)]
    for i in range(hist_len):
        low[i][i] = low[i][i] + ridge
    inverse = [None] * hist_len
    factor = [[None] * hist_len for _ in range(hist_len)]
    forward = [jnp.ones_like(trace) for _ in range(hist_len)]
    for j in range(hist_len):
        inverse[j] = 1.0 / low[j][j]
        for i in range(j + 1, hist_len):
            factor[i][j] = low[i][j] * inverse[j]
        for i in range(j + 1, hist_len):
            forward[i] = forward[i] - factor[i][j] * forward[j]
            for k in range(j + 1, i + 1):
                low[i][k] = low[i][k] - factor[i][j] * low[k][j]
    backward = [forward[i] * inverse[i] for i in range(hist_len)]
    for j in reversed(range(hist_len)):
        for i in range(j):
            backward[i] = backward[i] - factor[j][i] * backward[j]
    total = backward[0]
    for i in range(1, hist_len):
        total = total + backward[i]
    return [backward[i] / total for i in range(hist_len)]


def split(x):
    pieces = []
    for _ in range(2):
        piece = x.astype(jnp.bfloat16).astype(F32)
        pieces.append(piece)
        x = x - piece
    return pieces


def flips(value, count):
    out = []
    bit = 1
    while bit < count:
        out.append(bit - 2 * bit * lax.rem(lax.div(value, bit), 2))
        bit *= 2
    return out


def flipped(value, changes, mask):
    for k, change in enumerate(changes):
        if mask >> k & 1:
            value = value + change
    return value


def kernel(
    cfg,
    batch_atom_hbm,
    owner_slot_hbm,
    slot_index_hbm,
    w_hbm,
    target_hbm,
    coupling_hbm,
    basis_hbm,
    rho_hbm,
    res_hbm,
    density_out,
    moments_out,
    w,
    target,
    coupling,
    basis,
    rho,
    res,
    fresh,
    row_bufs,
    sent_moments,
    all_moments,
    near,
    own,
    own_sum,
    halves,
    hist_moments,
    base_rows,
    batch_atom,
    owner_slot,
    slot_index,
    load_sem,
    row_sem,
    moment_sem,
):
    iters, hist_len, harmonics, batches, width, owned, groups, members, scale = cfg
    devices = groups * members
    tiles = w.shape[0]
    per_batch = width // LANES
    half = LANES // 2
    rows = batches // 4
    my_group = lax.axis_index("grid")
    my_member = lax.axis_index("atom")
    me = my_group * members + my_member
    chips = devices // 2
    upper = chips // 2
    chip = lax.div(me, 2)
    core = lax.rem(me, 2)
    group_flips = flips(my_group, groups)
    member_flips = flips(my_member, members)

    def peer(step):
        return (
            flipped(my_group, group_flips, step // members),
            flipped(my_member, member_flips, step % members),
        )

    plane = min(chips, (members // 2) ** 2)
    chip_steps = [z * plane + p for p in reversed(range(plane)) for z in reversed(range(chips // plane))]
    device_steps = [2 * step + c for c in (0, 1) for step in chip_steps]
    device_steps.remove(0)

    barrier = pltpu.get_barrier_semaphore()

    loads = [
        pltpu.make_async_copy(src, dst, load_sem.at[k])
        for k, (src, dst) in enumerate(
            (
                (res_hbm, res),
                (w_hbm, w),
                (basis_hbm, basis),
                (rho_hbm, rho),
                (target_hbm, target),
                (coupling_hbm, coupling),
                (batch_atom_hbm, batch_atom),
                (owner_slot_hbm, owner_slot),
                (slot_index_hbm, slot_index),
            )
        )
    ]
    for k in (6, 7, 0, 1):
        loads[k].start()

    for step in device_steps:
        pl.semaphore_signal(barrier, inc=1, device_id=peer(step), device_id_type=MESH)

    for k in (2, 3, 4, 5, 8):
        loads[k].start()
    loads[6].wait()
    loads[7].wait()

    lane = lax.broadcasted_iota(jnp.int32, (SUBS, LANES), 1)
    sub = lax.broadcasted_iota(jnp.int32, (SUBS, LANES), 0)
    quarter = lane // 32
    lane_row = lax.broadcasted_iota(jnp.int32, (1, LANES), 1)

    slot_row = jnp.zeros((1, LANES), F32)
    slot_cols = []
    for block in range(batches // SUBS):
        col = jnp.zeros((SUBS, LANES), F32)
        for at in range(SUBS):
            b = block * SUBS + at
            slot = owner_slot[batch_atom[b]].astype(F32)
            slot_row = jnp.where(lane_row == half + b, slot, slot_row)
            col = jnp.where(sub == at, slot, col)
        slot_cols.append(col)
    slot_col = jnp.concatenate(slot_cols, axis=0)

    def lane_tile(t):
        return pl.ds(pl.multiple_of(t * LANES, LANES), LANES)

    def remote(src, dst, sems, step):
        return pltpu.make_async_remote_copy(
            src_ref=src,
            dst_ref=dst,
            send_sem=sems.at[0],
            recv_sem=sems.at[1],
            device_id=peer(step),
            device_id_type=MESH,
        )

    def exchange_rows(buf, sems):
        for step in device_steps:
            remote(buf.at[me], buf.at[me], sems, step).start()

        def wait():
            others = buf.at[pl.ds(0, devices - 1)]
            everyone = remote(others, others, sems, 1)
            everyone.wait_recv()
            everyone.wait_send()

        return wait

    def exchange_moments(mine, buf, sems, favour):
        halves = [pl.ds((upper * k + chip - lax.rem(chip, upper)) % chips, upper) for k in range(2)]
        remote(mine, buf.at[0, chip], sems.at[0], 1).start()
        def send(step):
            remote(mine, buf.at[0, chip], sems.at[step // upper], 2 * step + 1).start()

        if favour:
            origin = pltpu.make_async_remote_copy(
                src_ref=mine,
                dst_ref=buf.at[0, chip],
                send_sem=sems.at[lax.div(chip, upper), 0],
                recv_sem=sems.at[lax.div(chip, upper), 1],
                device_id=(0, 1 - core),
                device_id_type=MESH,
            )
            pl.when(chip != 0)(origin.start)
            for step in chip_steps[:-1]:
                pl.when(chip != step)(functools.partial(send, step))
        else:
            for step in chip_steps[:-1]:
                send(step)
        landed = [remote(buf.at[0, half], buf.at[0, half], sems.at[k], 1) for k, half in enumerate(halves)]
        passed = [remote(buf.at[0, half], buf.at[1, half], sems.at[2 + k], 1) for k, half in enumerate(halves)]

        def wait_landed():
            for k in range(2):
                landed[k].wait_recv()
                passed[k].start()

        def wait_passed():
            for k in range(2):
                passed[k].wait_recv()
            for k in range(2):
                landed[k].wait_send()
                passed[k].wait_send()

        return wait_landed, wait_passed

    def total_row(buf):
        parts = [buf[spot] for spot in range(devices)]
        while len(parts) > 1:
            parts = [parts[k] + parts[k + 1] for k in range(0, len(parts), 2)]
        return parts[0]

    def splat(row, k):
        return jnp.broadcast_to(row[:, k : k + 1], (1, LANES))

    shifts = hist_len // 2 + 1
    entry = None
    for iteration in range(iters):
        row_buf = row_bufs.at[iteration]
        sent_buf = sent_moments.at[iteration]
        moment_buf = all_moments.at[iteration]
        last = iteration == iters - 1

        if iteration == 0:
            loads[0].wait()
            loads[1].wait()

            def gram(step, acc):
                acc = list(acc)
                for u in range(8):
                    t = step * 8 + u
                    x = res[:, lane_tile(t)]
                    y = x * w[pl.ds(t, 1), :]
                    for r in range(shifts):
                        acc[r] = acc[r] + y * (pltpu.roll(x, r, 0) if r else x)
                return tuple(acc)

            acc = lax.fori_loop(0, tiles // 8, gram, tuple(jnp.zeros((SUBS, LANES), F32) for _ in range(shifts)))
            packed = jnp.zeros((SUBS, LANES), F32)
            for r in range(shifts):
                packed = jnp.where(lane == hist_len * r + sub, jnp.sum(acc[r], axis=1, keepdims=True), packed)
            row_buf[pl.ds(me, 1)] = (jnp.sum(packed, axis=0, keepdims=True) + slot_row)[None]
            pl.semaphore_wait(barrier, devices - 1)
        else:
            slot = slot_index[iteration - 1]
            replaced = sub == slot

            acc = (acc[0] + acc[1]) + (acc[2] + acc[3])
            square = jnp.sum(square, axis=0, keepdims=True)
            acc = jnp.where(replaced, square, acc)
            packed = jnp.where(lane == sub, jnp.sum(acc, axis=1, keepdims=True), 0.0)
            row_buf[pl.ds(me, 1)] = jnp.sum(packed, axis=0, keepdims=True)[None]
        wait = exchange_rows(row_buf, row_sem)

        if iteration == 0:
            loads[2].wait()
        else:

            @pl.loop(0, tiles // 8)
            def _(step):
                for u in range(8):
                    t = step * 8 + u
                    res[:, lane_tile(t)] = jnp.where(replaced, fresh[pl.ds(t, 1), :], res[:, lane_tile(t)])
                    rho[:, lane_tile(t)] = jnp.where(replaced, density_out[pl.ds(t, 1), :], rho[:, lane_tile(t)])

        @pl.loop(0, rows)
        def _(r):
            xs, ys = [], []
            for q in range(4):
                b = q * rows + r
                at = pl.ds(pl.multiple_of(b * width, width), width)
                gain = jnp.concatenate([w[pl.ds(b * per_batch + v, 1), :] for v in range(per_batch)], axis=1)
                xs.extend(split(res[:, at] * gain))
                slab = pl.ds(pl.multiple_of(b * 32, 32), 32)
                if iteration == 0:
                    y = jnp.concatenate([basis[0:24, at], jnp.broadcast_to(basis[24:25, at], (SUBS, width))], axis=0)
                    pair = [piece.astype(jnp.bfloat16) for piece in split(y)]
                    for k in range(2):
                        halves[k, slab, :] = pair[k]
                else:
                    pair = [halves[k, slab, :] for k in range(2)]
                ys.append(pair)
            x = jnp.concatenate(xs, axis=0).astype(jnp.bfloat16)
            out = None
            for k in range(2):
                y = jnp.concatenate([pair[k] for pair in ys], axis=0)
                part = lax.dot_general(x, y, (((1,), (1,)), ((), ())), preferred_element_type=F32)
                out = part if out is None else out + part
            tile = jnp.zeros((SUBS, LANES), F32)
            for q in range(4):
                block = out[16 * q : 16 * q + 8] + out[16 * q + 8 : 16 * q + 16]
                tile = jnp.where(quarter == q, block, tile)
            hist_moments[r] = tile

        wait()

        row = total_row(row_buf)
        if iteration == 0:
            entry = [[None] * (i + 1) for i in range(hist_len)]
            for i in range(hist_len):
                for j in range(i + 1):
                    r = i - j
                    at = hist_len * r + i if r < shifts else hist_len * (hist_len - r) + j
                    entry[i][j] = splat(row, at)
        else:
            news = [splat(row, k) for k in range(hist_len)]
            slot_vec = jnp.zeros((1, LANES), jnp.int32) + slot
            entry = [
                [
                    jnp.where(slot_vec == i, news[j], jnp.where(slot_vec == j, news[i], entry[i][j]))
                    for j in range(i + 1)
                ]
                for i in range(hist_len)
            ]
        coeffs = solve_coeffs(entry, hist_len)
        coeff_col = jnp.zeros((SUBS, LANES), F32)
        for i in range(hist_len):
            coeff_col = jnp.where(sub == i, coeffs[i], coeff_col)

        mixed = [jnp.sum(coeff_col * hist_moments[r], axis=0, keepdims=True) for r in range(rows)]
        sent_buf[...] = jnp.concatenate(mixed, axis=0)
        wait_landed, wait_passed = exchange_moments(sent_buf, moment_buf, moment_sem, True)

        if iteration == 0:
            base = (my_member * owned).astype(F32)
            wide = lax.broadcasted_iota(jnp.int32, (owned, LANES), 0).astype(F32) + base

            @pl.loop(0, devices // SUBS)
            def _(c):
                side = lax.div(c, chips // SUBS)
                first = 2 * SUBS * lax.rem(c, chips // SUBS) + lax.rem(core + 1 + side, 2)
                ids = jnp.concatenate([row_buf[first + 2 * i] for i in range(SUBS)], axis=0)
                stepped = pltpu.roll(ids, 0, 1, stride=rows, stride_axis=0)
                for q in range(4):
                    turned = pltpu.roll(stepped, (half - rows * q) % LANES, 1)
                    slots = jnp.sum(jnp.where(lane // rows == sub, turned, 0.0), axis=0, keepdims=True)
                    near[q * batches : (q + 1) * batches, lane_tile(c)] = jnp.where(
                        slot_col == slots, 1.0, 0.0
                    ).astype(jnp.bfloat16)
                    own[:, lane_tile(4 * c + q)] = jnp.where(wide == slots, 1.0, 0.0).astype(jnp.bfloat16)

            for k in (3, 4, 5, 8):
                loads[k].wait()

        def base_step(step, carry):
            for u in range(8):
                t = step * 8 + u
                part = coeff_col * (rho[:, lane_tile(t)] + mixing_beta * res[:, lane_tile(t)])
                base_rows[pl.ds(t, 1), :] = jnp.sum(part, axis=0, keepdims=True)
            return carry

        lax.fori_loop(0, tiles // 8, base_step, 0)
        depth = chips * rows

        def pieces_of(side):
            everywhere = moment_buf[side].reshape(depth, LANES)
            return jnp.concatenate([piece.astype(jnp.bfloat16) for piece in split(everywhere)], axis=1)

        def near_part(pieces, side):
            group = lax.broadcasted_iota(jnp.int32, (batches, LANES), 1) // 32
            total = None
            for half in range(2):
                lines = slice(2 * half * batches, 2 * (half + 1) * batches)
                out = jnp.dot(near[lines, side * depth : (side + 1) * depth], pieces, preferred_element_type=F32)
                out = out[:, 0:LANES] + out[:, LANES:]
                pair = jnp.where(group % 2 == 0, out[0:batches], out[batches:])
                total = pair if half == 0 else jnp.where(group // 2 == 0, total, pair)
            return total

        def own_part(pieces, side):
            turn = lax.broadcasted_iota(jnp.int32, (1, 2 * LANES), 1) % LANES // 32
            picks = [jnp.where(turn == q, 1.0, 0.0).astype(jnp.bfloat16) for q in range(4)]
            stacked = jnp.concatenate(
                [pieces[c : c + LANES] * pick for c in range(0, depth, LANES) for pick in picks], axis=0
            )
            outs = []
            for k in range(2):
                mine = own[k * owned // 2 : (k + 1) * owned // 2, 4 * side * depth : 4 * (side + 1) * depth]
                out = jnp.dot(mine, stacked, preferred_element_type=F32)
                outs.append(out[:, 0:LANES] + out[:, LANES:])
            return jnp.concatenate(outs, axis=0)

        def folded(total):
            total = total + pltpu.roll(total, 64, 1)
            return (total + pltpu.roll(total, 32, 1)) * scale

        wait_landed()
        pieces = pieces_of(0)
        near_sum = near_part(pieces, 0)
        if last:
            own_sum[...] = own_part(pieces, 0)
        wait_passed()
        pieces = pieces_of(1)
        near_sum = near_sum + near_part(pieces, 1)
        if last:
            own_sum[...] = own_sum[...] + own_part(pieces, 1)
        at_batch = folded(near_sum)
        comp = lax.broadcasted_iota(jnp.int32, (batches, LANES), 1) % 32
        spot = lax.broadcasted_iota(jnp.int32, (batches, LANES), 0) % SUBS
        turn = lax.broadcasted_iota(jnp.int32, (batches, LANES), 1) // 32
        degree = sum((comp >= (l + 1) * (l + 1)).astype(F32) for l in range(4))
        damped = jnp.where(comp < harmonics, at_batch * (mixing_beta / (1.0 + degree)), 0.0)
        spread = jnp.concatenate([jnp.where(spot == turn + 4 * side, damped, 0.0) for side in range(2)], axis=1)
        high, low = split(spread)
        acc = [jnp.zeros((SUBS, LANES), F32) for _ in range(4)]
        square = jnp.zeros((SUBS, LANES), F32)
        for g in range(batches // SUBS):
            mine = slice(g * SUBS, (g + 1) * SUBS)
            x = jnp.concatenate([high[mine], low[mine]], axis=0).astype(jnp.bfloat16)
            out = None
            for k in range(2):
                y = halves[k, g * SUBS * 32 : (g + 1) * SUBS * 32, :]
                part = jnp.dot(x, y, preferred_element_type=F32)
                out = part if out is None else out + part
            out = out[0:SUBS] + out[SUBS:]
            for v in range(per_batch):
                lines = pl.ds(g * SUBS * per_batch + v, SUBS, stride=per_batch)
                density = base_rows[lines, :] - out[:, v * LANES : (v + 1) * LANES]
                density_out[lines, :] = density
                if not last:
                    new = target[lines, :] + coupling[lines, :] * jnp.tanh(density) - density
                    new_w = new * w[lines, :]
                    fresh[lines, :] = new
                    square = square + new * new_w
                    for k in range(SUBS):
                        t = (g * SUBS + k) * per_batch + v
                        line = jnp.broadcast_to(new_w[k : k + 1, :], (SUBS, LANES))
                        acc[k % 4] = acc[k % 4] + line * res[:, t * LANES : (t + 1) * LANES]
        if last:
            turned = jnp.transpose(own_sum[...])
            final = (turned[0:32] + turned[32:64]) + (turned[64:96] + turned[96:128])
            moments_out[...] = final[0:harmonics] * scale


def finish(density, moments, density_out, moments_out, sem):
    copies = [
        pltpu.make_async_copy(density, density_out, sem.at[0]),
        pltpu.make_async_copy(moments, moments_out, sem.at[1]),
    ]
    for copy in copies:
        copy.start()
    for copy in copies:
        copy.wait()


def local(weights, target, coupling, multipole_basis, rho_hist, res_hist, batch_atom, owner_slot, slot_index):
    harmonics, points = multipole_basis.shape
    hist_len = res_hist.shape[0]
    batches = batch_atom.shape[0]
    groups = lax.axis_size("grid")
    members = lax.axis_size("atom")
    devices = groups * members
    owned = owner_slot.shape[0] // members
    scale = 1.0 / math.sqrt(points * groups // owned)
    iters = slot_index.shape[0]
    cfg = (iters, hist_len, harmonics, batches, points // batches, owned, groups, members, scale)
    tiles = points // LANES
    flat = (tiles, LANES)
    any_space = pl.BlockSpec(memory_space=pl.ANY)
    vmem = pl.BlockSpec(memory_space=pltpu.VMEM)
    density, moments = pl.pallas_call(
        functools.partial(kernel, cfg),
        out_shape=(jax.ShapeDtypeStruct(flat, F32), jax.ShapeDtypeStruct((harmonics, owned), F32)),
        in_specs=[any_space] * 9,
        out_specs=(vmem, vmem),
        scratch_shapes=[
            pltpu.VMEM(flat, F32),
            pltpu.VMEM(flat, F32),
            pltpu.VMEM(flat, F32),
            pltpu.VMEM((harmonics, points), F32),
            pltpu.VMEM((hist_len, points), F32),
            pltpu.VMEM((hist_len, points), F32),
            pltpu.VMEM(flat, F32),
            pltpu.VMEM((iters, devices, 1, LANES), F32),
            pltpu.VMEM((iters, batches // 4, LANES), F32),
            pltpu.VMEM((iters, 2, devices // 2, batches // 4, LANES), F32),
            pltpu.VMEM((4 * batches, devices * batches // 4), jnp.bfloat16),
            pltpu.VMEM((owned, devices * batches), jnp.bfloat16),
            pltpu.VMEM((owned, LANES), F32),
            pltpu.VMEM((2, batches * 32, points // batches), jnp.bfloat16),
            pltpu.VMEM((batches // 4, SUBS, LANES), F32),
            pltpu.VMEM(flat, F32),
            pltpu.SMEM(batch_atom.shape, batch_atom.dtype),
            pltpu.SMEM(owner_slot.shape, owner_slot.dtype),
            pltpu.SMEM(slot_index.shape, slot_index.dtype),
            pltpu.SemaphoreType.DMA((9,)),
            pltpu.SemaphoreType.DMA((2,)),
            pltpu.SemaphoreType.DMA((4, 2)),
        ],
        compiler_params=pltpu.CompilerParams(
            collective_id=0, has_side_effects=True, vmem_limit_bytes=40 * 1024 * 1024
        ),
    )(
        *(
            pltpu.with_memory_space_constraint(x, pltpu.HBM)
            for x in (
                batch_atom,
                owner_slot,
                slot_index,
                weights.reshape(flat),
                target.reshape(flat),
                coupling.reshape(flat),
                multipole_basis,
                rho_hist,
                res_hist,
            )
        )
    )
    density, moments = pl.pallas_call(
        finish,
        out_shape=(jax.ShapeDtypeStruct(flat, F32), jax.ShapeDtypeStruct((harmonics, owned), F32)),
        in_specs=[vmem] * 2,
        out_specs=(any_space, any_space),
        scratch_shapes=[pltpu.SemaphoreType.DMA((2,))],
    )(*(pltpu.with_memory_space_constraint(x, pltpu.VMEM) for x in (density, moments)))
    return density.reshape(points), moments


def solution(mesh):
    both = ("grid", "atom")
    placed = (P(both), P(both), P(both), P(None, both), P(None, both), P(None, both), P(both), P(), P())
    return jax.shard_map(
        local,
        mesh=mesh,
        in_specs=placed,
        out_specs=(P(both), P(None, "atom")),
        check_vma=False,
    )
```
